32 devices in a mesh: batch: 1 (over z), cols: 4 (over y), rows: 8 (over x, core).
Axes of the slice: x: 4, y: 4, z: 1, core: 2. Of those that a mesh axis runs over, the one named last changes fastest.
The devices are a block of a 4x4x8 slice.
Arguments:
- frames: bfloat16 [16, 1, 256, 384, 8], P(None, 'batch', 'rows', 'cols')
- h_init: float32 [1, 256, 384, 64], P('batch', 'rows', 'cols')
- w_x: bfloat16 [3, 3, 8, 192], replicated
- w_hzr: bfloat16 [3, 3, 64, 128], replicated
- w_hn: bfloat16 [3, 3, 64, 64], replicated
- gate_bias: float32 [192], replicated
Outputs:
- output 1: bfloat16 [16, 1, 256, 384, 64], P(None, 'batch', 'rows', 'cols')
- output 2: float32 [1, 256, 384, 64], P('batch', 'rows', 'cols')
All inputs are finite; a program needn't handle non-finite values.
Results may differ from the reference program's by a relative error of at most 0.00386505.
Values are sent between devices in bfloat16 or wider.
A program may use at most 768 MiB of HBM per device.

```python
import jax
import jax.numpy as jnp
from jax import lax

STEPS = 16
BATCH = 1
HEIGHT = 256
WIDTH = 384
CIN = 8
CH = 64


def setup_inputs(seed: int = 0, part: int = 0) -> dict:
    keys = jax.random.split(jax.random.key(seed), 6)
    key_frames = jax.random.fold_in(keys[0], part)
    key_state = jax.random.fold_in(keys[1], part)
    frames = jax.random.normal(key_frames, (STEPS, BATCH, HEIGHT, WIDTH, CIN), jnp.float32).astype(jnp.bfloat16)
    h_init = 0.8 * jax.random.normal(key_state, (BATCH, HEIGHT, WIDTH, CH), jnp.float32)
    w_x = (jax.random.normal(keys[2], (3, 3, CIN, 3 * CH), jnp.float32) * (9 * CIN) ** -0.5).astype(jnp.bfloat16)
    w_hzr = (jax.random.normal(keys[3], (3, 3, CH, 2 * CH), jnp.float32) * (1.5 * (9 * CH) ** -0.5)).astype(jnp.bfloat16)
    w_hn = (jax.random.normal(keys[4], (3, 3, CH, CH), jnp.float32) * (2.0 * (9 * CH) ** -0.5)).astype(jnp.bfloat16)
    gate_bias = 0.5 * jax.random.normal(keys[5], (3 * CH,), jnp.float32)
    return {'frames': frames, 'h_init': h_init, 'w_x': w_x, 'w_hzr': w_hzr, 'w_hn': w_hn, 'gate_bias': gate_bias}


def conv_same(inputs, weights):
    return lax.conv_general_dilated(inputs.astype(jnp.float32), weights.astype(jnp.float32), (1, 1), 'SAME', dimension_numbers=('NHWC', 'HWIO', 'NHWC'), precision=lax.Precision.HIGHEST)


def reference(frames, h_init, w_x, w_hzr, w_hn, gate_bias):
    def one_step(h_prev, frame_t):
        gate_x = conv_same(frame_t, w_x) + gate_bias
        zr_gates = jax.nn.sigmoid(gate_x[..., :2 * CH] + conv_same(h_prev.astype(jnp.bfloat16), w_hzr))
        update = zr_gates[..., :CH]
        reset_hid = (zr_gates[..., CH:] * h_prev).astype(jnp.bfloat16)
        candidate = jnp.tanh(gate_x[..., 2 * CH:] + conv_same(reset_hid, w_hn))
        h_next = (1.0 - update) * candidate + update * h_prev
        return h_next, h_next.astype(jnp.bfloat16)
    h_last, h_seq = lax.scan(one_step, h_init, frames)
    return h_seq, h_last
```

```python
import functools

import jax
import jax.numpy as jnp
from jax import lax
from jax.experimental import pallas as pl
from jax.experimental.pallas import tpu as pltpu
from jax.sharding import PartitionSpec as P

FUSE = 2
CHUNK = 4
MARGIN = 16
COMP = 112
DIRS = ((-1, 0), (1, 0), (0, -1), (0, 1), (-1, -1), (-1, 1), (1, -1), (1, 1))


def frames_with_halo(frames, width, n_rows, n_cols):
    down = [(i, i + 1) for i in range(n_rows - 1)]
    up = [(i + 1, i) for i in range(n_rows - 1)]
    above = lax.ppermute(frames[:, -width:], 'rows', down)
    below = lax.ppermute(frames[:, :width], 'rows', up)
    tall = jnp.concatenate([above, frames, below], axis=1)
    right = [(i, i + 1) for i in range(n_cols - 1)]
    left = [(i + 1, i) for i in range(n_cols - 1)]
    from_left = lax.ppermute(tall[..., -width:], 'cols', right)
    from_right = lax.ppermute(tall[..., :width], 'cols', left)
    return jnp.concatenate([from_left, tall, from_right], axis=-1)


def fold_rows(w, order):
    n_gates = w.shape[-1] // 64
    blocks = []
    for rho in order:
        outs = []
        for o in range(2):
            a = rho - o + 1
            outs.append(w[a] if 0 <= a <= 2 else jnp.zeros_like(w[0]))
        both = jnp.stack([b.reshape(3, w.shape[2], n_gates, 64) for b in outs], axis=3)
        blocks.append(both.reshape(3, w.shape[2], n_gates * 128))
    return jnp.stack(blocks, axis=1)


def kernel(dims, x_ref, h_ref, wzr_ref, wn_ref, b_ref, seq_ref, last_ref,
           hs, rh, zs, xl, stage, row_in, col_in, cor_in, send_sem, recv_sem, out_sem):
    n_steps, n_pairs, width, n_rows, n_cols = dims
    k = FUSE
    first = k + 1
    my_row = lax.axis_index('rows')
    my_col = lax.axis_index('cols')

    def there(di, dj):
        r, c = my_row + di, my_col + dj
        return jnp.logical_and(jnp.logical_and(r >= 0, r < n_rows), jnp.logical_and(c >= 0, c < n_cols))

    barrier = pltpu.get_barrier_semaphore()
    for di, dj in DIRS:
        @pl.when(there(di, dj))
        def _():
            pl.semaphore_signal(barrier, inc=1, device_id={'rows': my_row + di, 'cols': my_col + dj},
                                device_id_type=pl.DeviceIdType.MESH)

    hs[...] = jnp.zeros_like(hs)
    rh[...] = jnp.zeros_like(rh)
    for q in range(n_pairs):
        hs[first + q, MARGIN:MARGIN + width, :] = h_ref[q].T

    n_peers = sum(there(di, dj).astype(jnp.int32) for di, dj in DIRS)
    pl.semaphore_wait(barrier, n_peers)

    def src_of(di, dj):
        rows = {-1: pl.ds(first, k), 1: pl.ds(first + n_pairs - k, k), 0: pl.ds(first, n_pairs)}[di]
        cols = {-1: pl.ds(MARGIN, 8), 1: pl.ds(MARGIN + width - 8, 8), 0: pl.ds(MARGIN, width)}[dj]
        return rows, cols

    def dst_of(di, dj):
        rows = {-1: pl.ds(first + n_pairs, k), 1: pl.ds(first - k, k), 0: pl.ds(first, n_pairs)}[di]
        cols = {-1: pl.ds(MARGIN + width, 8), 1: pl.ds(MARGIN - 8, 8), 0: pl.ds(MARGIN, width)}[dj]
        return rows, cols

    def landing(d, par):
        if d < 2:
            return row_in.at[par, d]
        if d < 4:
            return col_in.at[par, d - 2]
        return cor_in.at[par, d - 4]

    def copy_of(d, par):
        di, dj = DIRS[d]
        rows, cols = src_of(di, dj)
        return pltpu.make_async_remote_copy(
            src_ref=hs.at[rows, cols, :], dst_ref=landing(d, par), send_sem=send_sem.at[d],
            recv_sem=recv_sem.at[par, d], device_id={'rows': my_row + di, 'cols': my_col + dj},
            device_id_type=pl.DeviceIdType.MESH)

    lane = lax.broadcasted_iota(jnp.int32, (1, 1, 128), 2)
    low = lane < 64

    def conv(src, s, q0, n, w_ref):
        parts = []
        for c in range(3):
            cols = pl.ds(MARGIN - 9 + c, COMP)
            own = src[q0:q0 + n, cols, :]
            edge = jnp.where(low, src[q0 + 1:q0 + 1 + n, cols, :], src[q0 - 1:q0 - 1 + n, cols, :])
            parts += [own.astype(jnp.bfloat16), edge.astype(jnp.bfloat16)]
        parts.append(xl[s, q0 - 1:q0 - 1 + n])
        lhs = jnp.concatenate(parts, axis=-1).reshape(n * COMP, 7 * 128)
        return jnp.dot(lhs, w_ref[...], preferred_element_type=jnp.float32)

    def sigmoid(v):
        return 0.5 * jnp.tanh(0.5 * v) + 0.5

    def zr_chunk(s, q0, n):
        acc = conv(hs, s, q0, n, wzr_ref)
        z = sigmoid(acc[:, :128] + b_ref[0:1, :])
        r = sigmoid(acc[:, 128:] + b_ref[1:2, :])
        zs[q0:q0 + n] = z.reshape(n, COMP, 128)
        rh[q0:q0 + n, MARGIN - 8:MARGIN - 8 + COMP, :] = r.reshape(n, COMP, 128) * hs[q0:q0 + n, MARGIN - 8:MARGIN - 8 + COMP, :]

    def n_chunk(s, q0, n, slot, last):
        acc = conv(rh, s, q0, n, wn_ref)
        cand = jnp.tanh(acc + b_ref[2:3, :]).reshape(n, COMP, 128)
        h = hs[q0:q0 + n, MARGIN - 8:MARGIN - 8 + COMP, :]
        h_new = cand + zs[q0:q0 + n] * (h - cand)
        inner = h_new[:, 8:8 + width, :]
        if last:
            hs[q0:q0 + n, MARGIN:MARGIN + width, :] = inner
        else:
            hs[q0:q0 + n, MARGIN - 8:MARGIN - 8 + COMP, :] = h_new
        for i in range(n):
            q = q0 + i - first
            if 0 <= q < n_pairs:
                stage[slot, q] = inner[i].T.astype(jnp.bfloat16)

    def chunks(lo, hi):
        for q0 in range(lo, hi, CHUNK):
            yield q0, min(CHUNK, hi - q0)

    def build_x(t, s):
        x = x_ref[t].astype(jnp.float32)
        taps = (pltpu.roll(x, 1, 1).astype(jnp.bfloat16), x_ref[t], pltpu.roll(x, 127, 1).astype(jnp.bfloat16))
        zero = jnp.zeros((32, 128), jnp.bfloat16)
        for i in range(n_pairs + 2 * k):
            both = jnp.concatenate([tap[16 * i:16 * i + 32] for tap in taps] + [zero], axis=0)
            xl[s, i] = both.T[:COMP]

    def out_copy(t, slot):
        return pltpu.make_async_copy(stage.at[slot], seq_ref.at[t], out_sem.at[slot])

    def period(p, carry):
        par = lax.rem(p, 2)
        for d, (di, dj) in enumerate(DIRS):
            @pl.when(there(di, dj))
            def _():
                copy_of(d, par).start()
        for s in range(k):
            build_x(p * k + s, s)
        for d, (di, dj) in enumerate(DIRS):
            @pl.when(there(-di, -dj))
            def _():
                copy_of(d, par).wait_recv()
                rows, cols = dst_of(di, dj)
                hs[rows, cols, :] = landing(d, par)[...]
        for s in range(k):
            ext = k - 1 - s
            t = p * k + s
            slot = s % 2 if k % 2 == 0 else lax.rem(t, 2)
            for q0, n in chunks(first - ext - 1, first + n_pairs + ext + 1):
                zr_chunk(s, q0, n)
            if s == 0:
                for d, (di, dj) in enumerate(DIRS):
                    @pl.when(there(di, dj))
                    def _():
                        copy_of(d, par).wait_send()

            @pl.when(t >= 2)
            def _():
                out_copy(t - 2, slot).wait()
            for q0, n in chunks(first - ext, first + n_pairs + ext):
                n_chunk(s, q0, n, slot, s == k - 1)
            out_copy(t, slot).start()
            if s < k - 1:
                @pl.when(my_row == 0)
                def _():
                    hs[first - ext:first, :, :] = jnp.zeros((ext, 128, 128), jnp.float32)

                @pl.when(my_row == n_rows - 1)
                def _():
                    hs[first + n_pairs:first + n_pairs + ext, :, :] = jnp.zeros((ext, 128, 128), jnp.float32)

                @pl.when(my_col == 0)
                def _():
                    hs[:, MARGIN - 8:MARGIN, :] = jnp.zeros((hs.shape[0], 8, 128), jnp.float32)

                @pl.when(my_col == n_cols - 1)
                def _():
                    hs[:, MARGIN + width:MARGIN + width + 8, :] = jnp.zeros((hs.shape[0], 8, 128), jnp.float32)
        return carry

    lax.fori_loop(0, n_steps // k, period, 0)
    for q in range(n_pairs):
        last_ref[q] = hs[first + q, MARGIN:MARGIN + width, :].T
    for t in range(n_steps - 2, n_steps):
        out_copy(t, t % 2).wait()


def solution(mesh):
    n_rows = mesh.shape['rows']
    n_cols = mesh.shape['cols']
    frame_spec = P(None, 'batch', 'rows', 'cols', None)
    state_spec = P('batch', 'rows', 'cols', None)

    def local_fn(frames, h_init, w_x, w_hzr, w_hn, gate_bias):
        n_steps, _, tile_h, width, c_in = frames.shape
        n_hidden = h_init.shape[-1]
        k = FUSE
        n_pairs = tile_h // 2
        halo = 2 * k
        x = frames_with_halo(frames[:, 0].transpose(0, 1, 3, 2), halo, n_rows, n_cols)
        x = jnp.pad(x, ((0, 0), (1, 1), (0, 0), (8 - halo, 128 - 8 - width - halo)))
        x = x.reshape(n_steps, (tile_h + 2 * halo + 2) * c_in, 128)
        h0 = h_init[0].transpose(0, 2, 1).reshape(n_pairs, 2 * n_hidden, width)
        wx = fold_rows(w_x, (-1, 0, 1, 2)).reshape(96, 384)
        wx = jnp.pad(wx, ((0, 32), (0, 0)))
        wzr = jnp.concatenate([fold_rows(w_hzr, (0, 1, 2, -1)).reshape(768, 256), wx[:, :256]], axis=0)
        wn = jnp.concatenate([fold_rows(w_hn, (0, 1, 2, -1)).reshape(768, 128), wx[:, 256:]], axis=0)
        bias = jnp.tile(gate_bias.reshape(3, 1, n_hidden), (1, 2, 1)).reshape(3, 128)
        n_buf = n_pairs + 2 * k + 2
        vmem = pl.BlockSpec(memory_space=pltpu.VMEM)
        seq, last = pl.pallas_call(
            functools.partial(kernel, (n_steps, n_pairs, width, n_rows, n_cols)),
            out_shape=(jax.ShapeDtypeStruct((n_steps, n_pairs, 128, width), jnp.bfloat16),
                       jax.ShapeDtypeStruct((n_pairs, 128, width), jnp.float32)),
            in_specs=[vmem] * 5,
            out_specs=(pl.BlockSpec(memory_space=pl.ANY), vmem),
            scratch_shapes=[
                pltpu.VMEM((n_buf, 128, 128), jnp.float32),
                pltpu.VMEM((n_buf, 128, 128), jnp.float32),
                pltpu.VMEM((n_buf, COMP, 128), jnp.float32),
                pltpu.VMEM((k, n_pairs + 2 * k, COMP, 128), jnp.bfloat16),
                pltpu.VMEM((2, n_pairs, 128, width), jnp.bfloat16),
                pltpu.VMEM((2, 2, k, width, 128), jnp.float32),
                pltpu.VMEM((2, 2, n_pairs, 8, 128), jnp.float32),
                pltpu.VMEM((2, 4, k, 8, 128), jnp.float32),
                pltpu.SemaphoreType.DMA((8,)),
                pltpu.SemaphoreType.DMA((2, 8)),
                pltpu.SemaphoreType.DMA((2,)),
            ],
            compiler_params=pltpu.CompilerParams(collective_id=0, has_side_effects=True),
        )(x, h0, wzr, wn, bias)
        seq = seq.reshape(n_steps, 1, tile_h, n_hidden, width).transpose(0, 1, 2, 4, 3)
        last = last.reshape(1, tile_h, n_hidden, width).transpose(0, 1, 3, 2)
        return seq, last

    return jax.shard_map(local_fn, mesh=mesh, in_specs=(frame_spec, state_spec, P(), P(), P(), P()), out_specs=(frame_spec, state_spec), check_vma=False)
```

```python
import functools

import jax
import jax.numpy as jnp
from jax import lax
from jax.experimental import pallas as pl
from jax.experimental.pallas import tpu as pltpu
from jax.sharding import PartitionSpec as P

FUSE = 2
CHUNK = 4
MARGIN = 16
COMP = 112
DIRS = ((-1, 0), (1, 0), (0, -1), (0, 1), (-1, -1), (-1, 1), (1, -1), (1, 1))


def kernel(dims, x_ref, h_ref, wx_raw, whzr_raw, whn_raw, bias_raw, seq_ref, last_ref,
           hs, rh, zs, xl, row_in, col_in, cor_in, wzr_ref, wn_ref, wx_ref, b_ref, xs, x_pack, x_row_in, x_col_in,
           send_sem, recv_sem, x_send_sem, x_recv_sem):
    n_steps, n_pairs, width, n_rows, n_cols = dims
    k = FUSE
    halo = 2 * k
    first = k + 1
    my_row = lax.axis_index('rows')
    my_col = lax.axis_index('cols')

    def there(di, dj):
        r, c = my_row + di, my_col + dj
        return jnp.logical_and(jnp.logical_and(r >= 0, r < n_rows), jnp.logical_and(c >= 0, c < n_cols))

    barrier = pltpu.get_barrier_semaphore()
    def greet(di, dj):
        @pl.when(there(di, dj))
        def _():
            pl.semaphore_signal(barrier, inc=1, device_id={'rows': my_row + di, 'cols': my_col + dj},
                                device_id_type=pl.DeviceIdType.MESH)

    x_row_in[...] = jnp.zeros_like(x_row_in)
    x_col_in[...] = jnp.zeros_like(x_col_in)
    for di, dj in DIRS:
        greet(di, dj)
    hs[...] = jnp.zeros_like(hs)
    rh[...] = jnp.zeros_like(rh)
    n_peers = sum(there(di, dj).astype(jnp.int32) for di, dj in DIRS)
    pl.semaphore_wait(barrier, n_peers)
    for q in range(n_pairs):
        hs[first + q, MARGIN:MARGIN + width, :] = h_ref[q].T

    def src_of(di, dj):
        rows = {-1: pl.ds(first, k), 1: pl.ds(first + n_pairs - k, k), 0: pl.ds(first, n_pairs)}[di]
        cols = {-1: pl.ds(MARGIN, 8), 1: pl.ds(MARGIN + width - 8, 8), 0: pl.ds(MARGIN, width)}[dj]
        return rows, cols

    def dst_of(di, dj):
        rows = {-1: pl.ds(first + n_pairs, k), 1: pl.ds(first - k, k), 0: pl.ds(first, n_pairs)}[di]
        cols = {-1: pl.ds(MARGIN + width, 8), 1: pl.ds(MARGIN - 8, 8), 0: pl.ds(MARGIN, width)}[dj]
        return rows, cols

    def landing(d, par):
        if d < 2:
            return row_in.at[par, d]
        if d < 4:
            return col_in.at[par, d - 2]
        return cor_in.at[par, d - 4]

    def copy_of(d, par):
        di, dj = DIRS[d]
        rows, cols = src_of(di, dj)
        return pltpu.make_async_remote_copy(
            src_ref=hs.at[rows, cols, :], dst_ref=landing(d, par), send_sem=send_sem.at[d],
            recv_sem=recv_sem.at[par, d], device_id={'rows': my_row + di, 'cols': my_col + dj},
            device_id_type=pl.DeviceIdType.MESH)

    lane = lax.broadcasted_iota(jnp.int32, (1, 1, 128), 2)
    low = lane < 64

    def conv(src, s, q0, n, w_ref):
        parts = []
        for c in range(3):
            cols = pl.ds(MARGIN - 9 + c, COMP)
            own = src[q0:q0 + n, cols, :]
            edge = jnp.where(low, src[q0 + 1:q0 + 1 + n, cols, :], src[q0 - 1:q0 - 1 + n, cols, :])
            parts += [own.astype(jnp.bfloat16), edge.astype(jnp.bfloat16)]
        parts.append(xl[s, q0 - 1:q0 - 1 + n])
        lhs = jnp.concatenate(parts, axis=-1).reshape(n * COMP, 7 * 128)
        return jnp.dot(lhs, w_ref[...], preferred_element_type=jnp.float32)

    def sigmoid(v):
        return 0.5 * jnp.tanh(0.5 * v) + 0.5

    def zr_chunk(s, q0, n):
        acc = conv(hs, s, q0, n, wzr_ref)
        z = sigmoid(acc[:, :128] + b_ref[0:1, :])
        r = sigmoid(acc[:, 128:] + b_ref[1:2, :])
        zs[q0:q0 + n] = z.reshape(n, COMP, 128)
        rh[q0:q0 + n, MARGIN - 8:MARGIN - 8 + COMP, :] = r.reshape(n, COMP, 128) * hs[q0:q0 + n, MARGIN - 8:MARGIN - 8 + COMP, :]

    def n_chunk(s, q0, n, t, last):
        acc = conv(rh, s, q0, n, wn_ref)
        cand = jnp.tanh(acc + b_ref[2:3, :]).reshape(n, COMP, 128)
        h = hs[q0:q0 + n, MARGIN - 8:MARGIN - 8 + COMP, :]
        h_new = cand + zs[q0:q0 + n] * (h - cand)
        inner = h_new[:, 8:8 + width, :]
        if last:
            hs[q0:q0 + n, MARGIN:MARGIN + width, :] = inner
        else:
            hs[q0:q0 + n, MARGIN - 8:MARGIN - 8 + COMP, :] = h_new
        for i in range(n):
            q = q0 + i - first
            if 0 <= q < n_pairs:
                seq_ref[t, q] = inner[i].T.astype(jnp.bfloat16)

    def chunks(lo, hi):
        for q0 in range(lo, hi, CHUNK):
            yield q0, min(CHUNK, hi - q0)

    n_sub = x_ref.shape[1]
    edge = halo * 8
    lane2 = lax.broadcasted_iota(jnp.int32, (1, 128), 1)

    def wide(v):
        return jnp.concatenate([v, jnp.zeros((v.shape[0], 128 - v.shape[1]), v.dtype)], axis=1)

    def x_copy(d):
        di, dj = DIRS[d]
        if dj == 0:
            src = x_ref.at[:, pl.ds(0 if di < 0 else n_sub - edge, edge), :]
            dst = x_row_in.at[0 if di < 0 else 1]
        else:
            rows = {-1: pl.ds(0, edge), 1: pl.ds(n_sub - edge, edge), 0: pl.ds(0, n_sub)}[di]
            there_rows = {-1: pl.ds(edge + n_sub, edge), 1: pl.ds(0, edge), 0: pl.ds(edge, n_sub)}[di]
            side = 0 if dj < 0 else 1
            src = x_pack.at[side, rows, :]
            dst = x_col_in.at[side, there_rows, :]
        return pltpu.make_async_remote_copy(
            src_ref=src, dst_ref=dst, send_sem=x_send_sem.at[d], recv_sem=x_recv_sem.at[d],
            device_id={'rows': my_row + di, 'cols': my_col + dj}, device_id_type=pl.DeviceIdType.MESH)

    def pack_x():
        x_pack[...] = jnp.zeros_like(x_pack)

        def add(t, carry):
            x = wide(x_ref[t].astype(jnp.float32))
            here = jnp.logical_and(lane2 >= 8 * t, lane2 < 8 * t + 8)
            x_pack[0] = jnp.where(here, pltpu.roll(x, 8 * t, 1), x_pack[0].astype(jnp.float32)).astype(jnp.bfloat16)
            x_pack[1] = jnp.where(here, pltpu.roll(x, lax.rem(8 * t + 128 - (width - 8), 128), 1), x_pack[1].astype(jnp.float32)).astype(jnp.bfloat16)
            return carry
        lax.fori_loop(0, n_steps, add, 0)

    def build_x(t, s):
        lo = lane2 < 8
        hi = lane2 >= 8 + width
        for first_sub, n, own, col in ((8, edge, x_row_in[1, t], 0), (8 + edge, n_sub, x_ref[t], edge), (8 + edge + n_sub, edge, x_row_in[0, t], edge + n_sub)):
            v = pltpu.roll(wide(own.astype(jnp.float32)), 8, 1)
            from_left = pltpu.roll(x_col_in[1, col:col + n, :].astype(jnp.float32), lax.rem(128 - 8 * t, 128), 1)
            from_right = pltpu.roll(x_col_in[0, col:col + n, :].astype(jnp.float32), lax.rem(128 + 8 + width - 8 * t, 128), 1)
            v = jnp.where(lo, from_left, jnp.where(hi, from_right, v))
            xs[0, first_sub:first_sub + n, :] = pltpu.roll(v, 1, 1)
            xs[1, first_sub:first_sub + n, :] = v
            xs[2, first_sub:first_sub + n, :] = pltpu.roll(v, 127, 1)
        zero = jnp.zeros((32, 128), jnp.bfloat16)
        for i in range(n_pairs + 2 * k):
            both = jnp.concatenate([xs[c, 16 * i:16 * i + 32].astype(jnp.bfloat16) for c in range(3)] + [zero], axis=0)
            xl[s, i] = both.T[:COMP]

    def fold_weights():
        def pair(get, a0, a1, gate):
            lo_part = get(a0, gate, 0) if 0 <= a0 <= 2 else None
            hi_part = get(a1, gate, 1) if 0 <= a1 <= 2 else None
            zero = jnp.zeros_like(lo_part if hi_part is None else hi_part)
            return jnp.where(lane2 < 64, zero if lo_part is None else lo_part, zero if hi_part is None else hi_part)

        for c in range(3):
            def get_h(a, gate, high):
                if gate == 2:
                    v = wide(whn_raw[a, c].astype(jnp.float32))
                    return pltpu.roll(v, 64, 1) if high else v
                v = whzr_raw[a, c].astype(jnp.float32)
                return pltpu.roll(v, 64, 1) if high != gate else v

            def get_x(a, gate, high):
                v = wx_raw[a, c].astype(jnp.float32)
                v = wide(v[:, 128:]) if gate == 2 else v[:, :128]
                return pltpu.roll(v, 64, 1) if high != (gate % 2) else v

            for j, rho in enumerate((0, 1, 2, -1)):
                at = c * 256 + j * 64
                for gate in range(2):
                    wzr_ref[at:at + 64, gate * 128:gate * 128 + 128] = pair(get_h, rho + 1, rho, gate).astype(jnp.bfloat16)
                wn_ref[at:at + 64, :] = pair(get_h, rho + 1, rho, 2).astype(jnp.bfloat16)
            for j, rho in enumerate((-1, 0, 1, 2)):
                at = c * 32 + j * 8
                for gate in range(3):
                    wx_ref[at:at + 8, gate * 128:gate * 128 + 128] = pair(get_x, rho + 1, rho, gate)
        wx_ref[96:128, :] = jnp.zeros((32, 384), jnp.float32)
        wzr_ref[768:896, :] = wx_ref[:, :256].astype(jnp.bfloat16)
        wn_ref[768:896, :] = wx_ref[:, 256:].astype(jnp.bfloat16)
        zr = bias_raw[:, :128]
        turned = pltpu.roll(zr, 64, 1)
        cand = wide(bias_raw[:, 128:])
        b_ref[0:1, :] = jnp.where(lane2 < 64, zr, turned)
        b_ref[1:2, :] = jnp.where(lane2 < 64, turned, zr)
        b_ref[2:3, :] = jnp.where(lane2 < 64, cand, pltpu.roll(cand, 64, 1))

    pack_x()
    for d, (di, dj) in enumerate(DIRS):
        @pl.when(there(di, dj))
        def _():
            x_copy(d).start()
    fold_weights()
    xs[...] = jnp.zeros_like(xs)
    for d, (di, dj) in enumerate(DIRS):
        @pl.when(there(-di, -dj))
        def _():
            x_copy(d).wait_recv()

    def period(p, carry):
        par = lax.rem(p, 2)
        for d, (di, dj) in enumerate(DIRS):
            @pl.when(there(di, dj))
            def _():
                copy_of(d, par).start()
        for s in range(k):
            build_x(p * k + s, s)
        for d, (di, dj) in enumerate(DIRS):
            @pl.when(there(-di, -dj))
            def _():
                copy_of(d, par).wait_recv()
                rows, cols = dst_of(di, dj)
                hs[rows, cols, :] = landing(d, par)[...]
        for s in range(k):
            ext = k - 1 - s
            t = p * k + s
            for q0, n in chunks(first - ext - 1, first + n_pairs + ext + 1):
                zr_chunk(s, q0, n)
            if s == 0:
                for d, (di, dj) in enumerate(DIRS):
                    @pl.when(there(di, dj))
                    def _():
                        copy_of(d, par).wait_send()

            for q0, n in chunks(first - ext, first + n_pairs + ext):
                n_chunk(s, q0, n, t, s == k - 1)
            if s < k - 1:
                @pl.when(my_row == 0)
                def _():
                    hs[first - ext:first, :, :] = jnp.zeros((ext, 128, 128), jnp.float32)

                @pl.when(my_row == n_rows - 1)
                def _():
                    hs[first + n_pairs:first + n_pairs + ext, :, :] = jnp.zeros((ext, 128, 128), jnp.float32)

                @pl.when(my_col == 0)
                def _():
                    hs[:, MARGIN - 8:MARGIN, :] = jnp.zeros((hs.shape[0], 8, 128), jnp.float32)

                @pl.when(my_col == n_cols - 1)
                def _():
                    hs[:, MARGIN + width:MARGIN + width + 8, :] = jnp.zeros((hs.shape[0], 8, 128), jnp.float32)
        return carry

    lax.fori_loop(0, n_steps // k, period, 0)
    for q in range(n_pairs):
        last_ref[q] = hs[first + q, MARGIN:MARGIN + width, :].T
    for d, (di, dj) in enumerate(DIRS):
        @pl.when(there(di, dj))
        def _():
            x_copy(d).wait_send()


def solution(mesh):
    n_rows = mesh.shape['rows']
    n_cols = mesh.shape['cols']
    frame_spec = P(None, 'batch', 'rows', 'cols', None)
    state_spec = P('batch', 'rows', 'cols', None)

    def local_fn(frames, h_init, w_x, w_hzr, w_hn, gate_bias):
        n_steps, _, tile_h, width, c_in = frames.shape
        n_hidden = h_init.shape[-1]
        k = FUSE
        n_pairs = tile_h // 2
        x = frames[:, 0].transpose(0, 1, 3, 2).reshape(n_steps, tile_h * c_in, width)
        h0 = h_init[0].transpose(0, 2, 1).reshape(n_pairs, 2 * n_hidden, width)
        edge = 2 * k * c_in
        n_buf = n_pairs + 2 * k + 2
        vmem = pl.BlockSpec(memory_space=pltpu.VMEM)
        seq, last = pl.pallas_call(
            functools.partial(kernel, (n_steps, n_pairs, width, n_rows, n_cols)),
            out_shape=(pltpu.VMEM((n_steps, n_pairs, 128, width), jnp.bfloat16),
                       jax.ShapeDtypeStruct((n_pairs, 128, width), jnp.float32)),
            in_specs=[vmem] * 6,
            out_specs=(vmem, vmem),
            scratch_shapes=[
                pltpu.VMEM((n_buf, 128, 128), jnp.float32),
                pltpu.VMEM((n_buf, 128, 128), jnp.float32),
                pltpu.VMEM((n_buf, COMP, 128), jnp.float32),
                pltpu.VMEM((k, n_pairs + 2 * k, COMP, 128), jnp.bfloat16),
                pltpu.VMEM((2, 2, k, width, 128), jnp.float32),
                pltpu.VMEM((2, 2, n_pairs, 8, 128), jnp.float32),
                pltpu.VMEM((2, 4, k, 8, 128), jnp.float32),
                pltpu.VMEM((896, 256), jnp.bfloat16),
                pltpu.VMEM((896, 128), jnp.bfloat16),
                pltpu.VMEM((128, 384), jnp.float32),
                pltpu.VMEM((3, 128), jnp.float32),
                pltpu.VMEM((3, tile_h * c_in + 2 * edge + 16, 128), jnp.float32),
                pltpu.VMEM((2, tile_h * c_in, 128), jnp.bfloat16),
                pltpu.VMEM((2, n_steps, edge, width), jnp.bfloat16),
                pltpu.VMEM((2, tile_h * c_in + 2 * edge, 128), jnp.bfloat16),
                pltpu.SemaphoreType.DMA((8,)),
                pltpu.SemaphoreType.DMA((2, 8)),
                pltpu.SemaphoreType.DMA((8,)),
                pltpu.SemaphoreType.DMA((8,)),
            ],
            compiler_params=pltpu.CompilerParams(collective_id=0, has_side_effects=True, vmem_limit_bytes=32 * 2**20),
        )(x, h0, w_x, w_hzr, w_hn, gate_bias.reshape(1, -1))
        seq = seq.reshape(n_steps, 1, tile_h, n_hidden, width).transpose(0, 1, 2, 4, 3)
        last = last.reshape(1, tile_h, n_hidden, width).transpose(0, 1, 3, 2)
        return seq, last

    return jax.shard_map(local_fn, mesh=mesh, in_specs=(frame_spec, state_spec, P(), P(), P(), P()), out_specs=(frame_spec, state_spec), check_vma=False)
```

```python
import functools

import jax
import jax.numpy as jnp
from jax import lax
from jax.experimental import pallas as pl
from jax.experimental.pallas import tpu as pltpu
from jax.sharding import PartitionSpec as P

FUSE = 2
CHUNK = 2
MARGIN = 16
COMP = 112
DIRS = ((-1, 0), (1, 0), (0, -1), (0, 1), (-1, -1), (-1, 1), (1, -1), (1, 1))


def kernel(dims, x_hbm, h_hbm, wx_hbm, whzr_hbm, whn_hbm, bias_hbm, seq_ref, last_ref,
           x_ref, h_ref, wx_raw, whzr_raw, whn_raw, bias_raw,
           hs, rh, zs, xl, row_in, col_in, cor_in, wzr_ref, wn_ref, wx_ref, b_ref, xs, x_pack, x_row_in, x_col_in,
           send_sem, recv_sem, x_send_sem, x_recv_sem, load_sem):
    n_steps, n_pairs, width, n_rows, n_cols = dims
    k = FUSE
    halo = 2 * k
    first = k + 1
    my_row = lax.axis_index('rows')
    my_col = lax.axis_index('cols')

    def there(di, dj):
        r, c = my_row + di, my_col + dj
        return jnp.logical_and(jnp.logical_and(r >= 0, r < n_rows), jnp.logical_and(c >= 0, c < n_cols))

    loads = [pltpu.make_async_copy(src, dst, load_sem.at[i]) for i, (src, dst) in enumerate(
        ((x_hbm, x_ref), (h_hbm, h_ref), (wx_hbm, wx_raw), (whzr_hbm, whzr_raw), (whn_hbm, whn_raw), (bias_hbm, bias_raw)))]
    for load in loads:
        load.start()
    barrier = pltpu.get_barrier_semaphore()
    def greet(di, dj):
        @pl.when(there(di, dj))
        def _():
            pl.semaphore_signal(barrier, inc=1, device_id={'rows': my_row + di, 'cols': my_col + dj},
                                device_id_type=pl.DeviceIdType.MESH)

    x_row_in[...] = jnp.zeros_like(x_row_in)
    x_col_in[...] = jnp.zeros_like(x_col_in)
    for di, dj in DIRS:
        greet(di, dj)
    hs[...] = jnp.zeros_like(hs)
    rh[...] = jnp.zeros_like(rh)
    n_peers = sum(there(di, dj).astype(jnp.int32) for di, dj in DIRS)
    pl.semaphore_wait(barrier, n_peers)
    moves = [(-1, 0, 0), (1, 0, 0)] + [(di, dj, 0) for di in (-1, 1) for dj in (-1, 1)]
    group = n_pairs // 4
    moves += [(0, dj, g) for g in range(4) for dj in (-1, 1)]
    sent_with = {0: (0, 2, 3, 6, 7), 1: (8, 9), 2: (10, 11), 3: (1, 4, 5, 12, 13)}

    def move(m, par):
        di, dj, g = moves[m]
        cols = {-1: pl.ds(MARGIN, halo), 1: pl.ds(MARGIN + width - halo, halo), 0: pl.ds(MARGIN, width)}[dj]
        if di == 0:
            src = hs.at[pl.ds(first + g * group, group), cols, :]
            dst = col_in.at[par, (dj + 1) // 2, pl.ds(g * group, group)]
        else:
            src = hs.at[pl.ds(first if di < 0 else first + n_pairs - k, k), cols, :]
            dst = row_in.at[par, (di + 1) // 2] if dj == 0 else cor_in.at[par, m - 2]
        return dst, pltpu.make_async_remote_copy(
            src_ref=src, dst_ref=dst, send_sem=send_sem.at[m], recv_sem=recv_sem.at[par, m],
            device_id={'rows': my_row + di, 'cols': my_col + dj}, device_id_type=pl.DeviceIdType.MESH)

    def send(g, par):
        for m in sent_with[g]:
            @pl.when(there(moves[m][0], moves[m][1]))
            def _():
                move(m, par)[1].start()

    def receive(g, par):
        for m in sent_with[g]:
            di, dj, _ = moves[m]

            @pl.when(there(-di, -dj))
            def _():
                dst, copy = move(m, par)
                copy.wait_recv()
                cols = {-1: pl.ds(MARGIN + width, halo), 1: pl.ds(MARGIN - halo, halo), 0: pl.ds(MARGIN, width)}[dj]
                rows = pl.ds(first + g * group, group) if di == 0 else pl.ds(first + n_pairs if di < 0 else first - k, k)
                hs[rows, cols, :] = dst[...]

    lane = lax.broadcasted_iota(jnp.int32, (1, 1, 128), 2)
    low = lane < 64

    def conv(src, s, q0, n, w_ref):
        parts = []
        for c in range(3):
            cols = pl.ds(MARGIN - 9 + c, COMP)
            own = src[q0:q0 + n, cols, :]
            edge = jnp.where(low, src[q0 + 1:q0 + 1 + n, cols, :], src[q0 - 1:q0 - 1 + n, cols, :])
            parts += [own.astype(jnp.bfloat16), edge.astype(jnp.bfloat16)]
        parts.append(xl[s, q0 - 1:q0 - 1 + n])
        lhs = jnp.concatenate(parts, axis=-1).reshape(n * COMP, 7 * 128)
        return jnp.dot(lhs, w_ref[...], preferred_element_type=jnp.float32)

    def sigmoid(v):
        return 0.5 * jnp.tanh(0.5 * v) + 0.5

    def zr_chunk(s, q0, n):
        acc = conv(hs, s, q0, n, wzr_ref)
        z = sigmoid(acc[:, :128] + b_ref[0:1, :])
        r = sigmoid(acc[:, 128:] + b_ref[1:2, :])
        zs[q0:q0 + n] = z.reshape(n, COMP, 128)
        rh[q0:q0 + n, MARGIN - 8:MARGIN - 8 + COMP, :] = r.reshape(n, COMP, 128) * hs[q0:q0 + n, MARGIN - 8:MARGIN - 8 + COMP, :]

    def n_chunk(s, q0, n, t, last):
        acc = conv(rh, s, q0, n, wn_ref)
        cand = jnp.tanh(acc + b_ref[2:3, :]).reshape(n, COMP, 128)
        h = hs[q0:q0 + n, MARGIN - 8:MARGIN - 8 + COMP, :]
        h_new = cand + zs[q0:q0 + n] * (h - cand)
        inner = h_new[:, 8:8 + width, :]
        if last:
            hs[q0:q0 + n, MARGIN:MARGIN + width, :] = inner
        else:
            hs[q0:q0 + n, MARGIN - 8:MARGIN - 8 + COMP, :] = h_new
        for i in range(n):
            q = q0 + i - first
            if 0 <= q < n_pairs:
                seq_ref[t, q] = inner[i].T.astype(jnp.bfloat16)

    def chunks(lo, hi):
        for q0 in range(lo, hi, CHUNK):
            yield q0, min(CHUNK, hi - q0)

    n_sub = x_ref.shape[1]
    edge = halo * 8
    lane2 = lax.broadcasted_iota(jnp.int32, (1, 128), 1)

    def wide(v):
        return jnp.concatenate([v, jnp.zeros((v.shape[0], 128 - v.shape[1]), v.dtype)], axis=1)

    def x_copy(d):
        di, dj = DIRS[d]
        if dj == 0:
            src = x_ref.at[:, pl.ds(0 if di < 0 else n_sub - edge, edge), :]
            dst = x_row_in.at[0 if di < 0 else 1]
        else:
            rows = {-1: pl.ds(0, edge), 1: pl.ds(n_sub - edge, edge), 0: pl.ds(0, n_sub)}[di]
            there_rows = {-1: pl.ds(edge + n_sub, edge), 1: pl.ds(0, edge), 0: pl.ds(edge, n_sub)}[di]
            side = 0 if dj < 0 else 1
            src = x_pack.at[side, rows, :]
            dst = x_col_in.at[side, there_rows, :]
        return pltpu.make_async_remote_copy(
            src_ref=src, dst_ref=dst, send_sem=x_send_sem.at[d], recv_sem=x_recv_sem.at[d],
            device_id={'rows': my_row + di, 'cols': my_col + dj}, device_id_type=pl.DeviceIdType.MESH)

    def pack_x():
        x_pack[...] = jnp.zeros_like(x_pack)

        def add(t, carry):
            x = wide(x_ref[t].astype(jnp.float32))
            here = jnp.logical_and(lane2 >= 8 * t, lane2 < 8 * t + 8)
            x_pack[0] = jnp.where(here, pltpu.roll(x, 8 * t, 1), x_pack[0].astype(jnp.float32)).astype(jnp.bfloat16)
            x_pack[1] = jnp.where(here, pltpu.roll(x, lax.rem(8 * t + 128 - (width - 8), 128), 1), x_pack[1].astype(jnp.float32)).astype(jnp.bfloat16)
            return carry
        lax.fori_loop(0, n_steps, add, 0)

    def build_x(t, s):
        lo = lane2 < 8
        hi = lane2 >= 8 + width
        for first_sub, n, own, col in ((8, edge, x_row_in[1, t], 0), (8 + edge, n_sub, x_ref[t], edge), (8 + edge + n_sub, edge, x_row_in[0, t], edge + n_sub)):
            v = pltpu.roll(wide(own.astype(jnp.float32)), 8, 1)
            from_left = pltpu.roll(x_col_in[1, col:col + n, :].astype(jnp.float32), lax.rem(128 - 8 * t, 128), 1)
            from_right = pltpu.roll(x_col_in[0, col:col + n, :].astype(jnp.float32), lax.rem(128 + 8 + width - 8 * t, 128), 1)
            v = jnp.where(lo, from_left, jnp.where(hi, from_right, v))
            xs[0, first_sub:first_sub + n, :] = pltpu.roll(v, 1, 1)
            xs[1, first_sub:first_sub + n, :] = v
            xs[2, first_sub:first_sub + n, :] = pltpu.roll(v, 127, 1)
        zero = jnp.zeros((32, 128), jnp.bfloat16)
        for i in range(n_pairs + 2 * k):
            both = jnp.concatenate([xs[c, 16 * i:16 * i + 32].astype(jnp.bfloat16) for c in range(3)] + [zero], axis=0)
            xl[s, i] = both.T[:COMP]

    def fold_weights():
        def pair(get, a0, a1, gate):
            lo_part = get(a0, gate, 0) if 0 <= a0 <= 2 else None
            hi_part = get(a1, gate, 1) if 0 <= a1 <= 2 else None
            zero = jnp.zeros_like(lo_part if hi_part is None else hi_part)
            return jnp.where(lane2 < 64, zero if lo_part is None else lo_part, zero if hi_part is None else hi_part)

        for c in range(3):
            def get_h(a, gate, high):
                if gate == 2:
                    v = wide(whn_raw[a, c].astype(jnp.float32))
                    return pltpu.roll(v, 64, 1) if high else v
                v = whzr_raw[a, c].astype(jnp.float32)
                return pltpu.roll(v, 64, 1) if high != gate else v

            def get_x(a, gate, high):
                v = wx_raw[a, c].astype(jnp.float32)
                v = wide(v[:, 128:]) if gate == 2 else v[:, :128]
                return pltpu.roll(v, 64, 1) if high != (gate % 2) else v

            for j, rho in enumerate((0, 1, 2, -1)):
                at = c * 256 + j * 64
                for gate in range(2):
                    wzr_ref[at:at + 64, gate * 128:gate * 128 + 128] = pair(get_h, rho + 1, rho, gate).astype(jnp.bfloat16)
                wn_ref[at:at + 64, :] = pair(get_h, rho + 1, rho, 2).astype(jnp.bfloat16)
            for j, rho in enumerate((-1, 0, 1, 2)):
                at = c * 32 + j * 8
                for gate in range(3):
                    wx_ref[at:at + 8, gate * 128:gate * 128 + 128] = pair(get_x, rho + 1, rho, gate)
        wx_ref[96:128, :] = jnp.zeros((32, 384), jnp.float32)
        wzr_ref[768:896, :] = wx_ref[:, :256].astype(jnp.bfloat16)
        wn_ref[768:896, :] = wx_ref[:, 256:].astype(jnp.bfloat16)
        zr = bias_raw[:, :128]
        turned = pltpu.roll(zr, 64, 1)
        cand = wide(bias_raw[:, 128:])
        b_ref[0:1, :] = jnp.where(lane2 < 64, zr, turned)
        b_ref[1:2, :] = jnp.where(lane2 < 64, turned, zr)
        b_ref[2:3, :] = jnp.where(lane2 < 64, cand, pltpu.roll(cand, 64, 1))

    loads[0].wait()
    pack_x()
    for d, (di, dj) in enumerate(DIRS):
        @pl.when(there(di, dj))
        def _():
            x_copy(d).start()
    loads[1].wait()
    for q in range(n_pairs):
        hs[first + q, MARGIN:MARGIN + width, :] = h_ref[q].T
    for g in (0, 3, 1, 2):
        send(g, 0)
    for load in loads[2:]:
        load.wait()
    fold_weights()
    xs[...] = jnp.zeros_like(xs)
    for d, (di, dj) in enumerate(DIRS):
        @pl.when(there(-di, -dj))
        def _():
            x_copy(d).wait_recv()

    def zr(s, lo, hi):
        for q0, n in chunks(first + lo, first + hi):
            zr_chunk(s, q0, n)

    def cand(t, s, lo, hi):
        for q0, n in chunks(first + lo, first + hi):
            n_chunk(s, q0, n, t, s == k - 1)

    n_periods = n_steps // k

    def period(p, carry):
        par = lax.rem(p, 2)
        for s in range(k):
            build_x(p * k + s, s)
        for s in range(k):
            ext = k - 1 - s
            t = p * k + s
            if s == 0:
                receive(0, par)
                receive(3, par)
                zr(s, -ext - 1, group - 1)
                zr(s, 3 * group + 1, n_pairs + ext + 1)
                receive(1, par)
                zr(s, group - 1, 2 * group - 1)
                receive(2, par)
                zr(s, 2 * group - 1, 3 * group + 1)
                for m, (di, dj, _) in enumerate(moves):
                    @pl.when(there(di, dj))
                    def _():
                        move(m, par)[1].wait_send()
            if s < k - 1:
                if s > 0:
                    zr(s, -ext - 1, n_pairs + ext + 1)
                cand(t, s, -ext, n_pairs + ext)

                @pl.when(my_row == 0)
                def _():
                    hs[first - ext:first, :, :] = jnp.zeros((ext, 128, 128), jnp.float32)

                @pl.when(my_row == n_rows - 1)
                def _():
                    hs[first + n_pairs:first + n_pairs + ext, :, :] = jnp.zeros((ext, 128, 128), jnp.float32)

                @pl.when(my_col == 0)
                def _():
                    hs[:, MARGIN - 8:MARGIN, :] = jnp.zeros((hs.shape[0], 8, 128), jnp.float32)

                @pl.when(my_col == n_cols - 1)
                def _():
                    hs[:, MARGIN + width:MARGIN + width + 8, :] = jnp.zeros((hs.shape[0], 8, 128), jnp.float32)
            else:
                more = p + 1 < n_periods

                def send_next(g):
                    @pl.when(more)
                    def _():
                        send(g, 1 - par)
                if s > 0:
                    zr(s, -1, group + 1)
                    zr(s, 3 * group - 1, n_pairs + 1)
                cand(t, s, 0, group)
                send_next(0)
                cand(t, s, 3 * group, n_pairs)
                send_next(3)
                if s > 0:
                    zr(s, group + 1, 3 * group - 1)
                cand(t, s, group, 2 * group)
                send_next(1)
                cand(t, s, 2 * group, 3 * group)
                send_next(2)
        return carry

    lax.fori_loop(0, n_steps // k, period, 0)
    for q in range(n_pairs):
        last_ref[q] = hs[first + q, MARGIN:MARGIN + width, :].T
    for d, (di, dj) in enumerate(DIRS):
        @pl.when(there(di, dj))
        def _():
            x_copy(d).wait_send()


def solution(mesh):
    n_rows = mesh.shape['rows']
    n_cols = mesh.shape['cols']
    frame_spec = P(None, 'batch', 'rows', 'cols', None)
    state_spec = P('batch', 'rows', 'cols', None)

    def local_fn(frames, h_init, w_x, w_hzr, w_hn, gate_bias):
        n_steps, _, tile_h, width, c_in = frames.shape
        n_hidden = h_init.shape[-1]
        k = FUSE
        n_pairs = tile_h // 2
        x = frames[:, 0].transpose(0, 1, 3, 2).reshape(n_steps, tile_h * c_in, width)
        h0 = h_init[0].transpose(0, 2, 1).reshape(n_pairs, 2 * n_hidden, width)
        edge = 2 * k * c_in
        n_buf = n_pairs + 2 * k + 2
        vmem = pl.BlockSpec(memory_space=pltpu.VMEM)
        seq, last = pl.pallas_call(
            functools.partial(kernel, (n_steps, n_pairs, width, n_rows, n_cols)),
            out_shape=(pltpu.VMEM((n_steps, n_pairs, 128, width), jnp.bfloat16),
                       jax.ShapeDtypeStruct((n_pairs, 128, width), jnp.float32)),
            in_specs=[pl.BlockSpec(memory_space=pltpu.HBM)] * 6,
            out_specs=(vmem, vmem),
            scratch_shapes=[
                pltpu.VMEM(x.shape, x.dtype),
                pltpu.VMEM(h0.shape, h0.dtype),
                pltpu.VMEM(w_x.shape, w_x.dtype),
                pltpu.VMEM(w_hzr.shape, w_hzr.dtype),
                pltpu.VMEM(w_hn.shape, w_hn.dtype),
                pltpu.VMEM((1, gate_bias.shape[0]), gate_bias.dtype),
                pltpu.VMEM((n_buf, 128, 128), jnp.float32),
                pltpu.VMEM((n_buf, 128, 128), jnp.float32),
                pltpu.VMEM((n_buf, COMP, 128), jnp.float32),
                pltpu.VMEM((k, n_pairs + 2 * k, COMP, 128), jnp.bfloat16),
                pltpu.VMEM((2, 2, k, width, 128), jnp.float32),
                pltpu.VMEM((2, 2, n_pairs, 2 * k, 128), jnp.float32),
                pltpu.VMEM((2, 4, k, 2 * k, 128), jnp.float32),
                pltpu.VMEM((896, 256), jnp.bfloat16),
                pltpu.VMEM((896, 128), jnp.bfloat16),
                pltpu.VMEM((128, 384), jnp.float32),
                pltpu.VMEM((3, 128), jnp.float32),
                pltpu.VMEM((3, tile_h * c_in + 2 * edge + 16, 128), jnp.float32),
                pltpu.VMEM((2, tile_h * c_in, 128), jnp.bfloat16),
                pltpu.VMEM((2, n_steps, edge, width), jnp.bfloat16),
                pltpu.VMEM((2, tile_h * c_in + 2 * edge, 128), jnp.bfloat16),
                pltpu.SemaphoreType.DMA((14,)),
                pltpu.SemaphoreType.DMA((2, 14)),
                pltpu.SemaphoreType.DMA((8,)),
                pltpu.SemaphoreType.DMA((8,)),
                pltpu.SemaphoreType.DMA((6,)),
            ],
            compiler_params=pltpu.CompilerParams(collective_id=0, has_side_effects=True, vmem_limit_bytes=32 * 2**20),
        )(*[pltpu.with_memory_space_constraint(v, pltpu.HBM) for v in (x, h0, w_x, w_hzr, w_hn, gate_bias.reshape(1, -1))])
        seq = seq.reshape(n_steps, 1, tile_h, n_hidden, width).transpose(0, 1, 2, 4, 3)
        last = last.reshape(1, tile_h, n_hidden, width).transpose(0, 1, 3, 2)
        return seq, last

    return jax.shard_map(local_fn, mesh=mesh, in_specs=(frame_spec, state_spec, P(), P(), P(), P()), out_specs=(frame_spec, state_spec), check_vma=False)
```

```python
import functools

import jax
import jax.numpy as jnp
from jax import lax
from jax.experimental import pallas as pl
from jax.experimental.pallas import tpu as pltpu
from jax.sharding import PartitionSpec as P

FUSE = 2
CHUNK = 2
N_CHUNK = 2
RIM = 4
MARGIN = 16
COMP = 112
DIRS = ((-1, 0), (1, 0), (0, -1), (0, 1), (-1, -1), (-1, 1), (1, -1), (1, 1))


def kernel(dims, x_hbm, h_hbm, wx_hbm, whzr_hbm, whn_hbm, bias_hbm, seq_ref, last_ref,
           x_ref, h_ref, wx_raw, whzr_raw, whn_raw, bias_raw,
           hs, rh, zs, xl, gate_zr, gate_n, row_in, col_in, cor_in, wzr_ref, wn_ref, wx_ref, wxzr_ref, wxn_ref, b_ref, xs, x_pack, x_row_in, x_col_in,
           send_sem, recv_sem, x_send_sem, x_recv_sem, load_sem):
    n_steps, n_pairs, width, n_rows, n_cols = dims
    k = FUSE
    halo = 2 * k
    first = k + 1
    my_row = lax.axis_index('rows')
    my_col = lax.axis_index('cols')

    def there(di, dj):
        r, c = my_row + di, my_col + dj
        return jnp.logical_and(jnp.logical_and(r >= 0, r < n_rows), jnp.logical_and(c >= 0, c < n_cols))

    loads = [pltpu.make_async_copy(src, dst, load_sem.at[i]) for i, (src, dst) in enumerate(
        ((x_hbm, x_ref), (h_hbm, h_ref), (wx_hbm, wx_raw), (whzr_hbm, whzr_raw), (whn_hbm, whn_raw), (bias_hbm, bias_raw)))]
    for load in loads:
        load.start()
    barrier = pltpu.get_barrier_semaphore()
    def device(di, dj):
        return (lax.axis_index('batch') * n_cols + my_col + dj) * n_rows + my_row + di

    def greet(di, dj):
        @pl.when(there(di, dj))
        def _():
            pl.semaphore_signal(barrier, inc=1, device_id=device(di, dj),
                                device_id_type=pl.DeviceIdType.LOGICAL)

    x_row_in[...] = jnp.zeros_like(x_row_in)
    x_col_in[...] = jnp.zeros_like(x_col_in)
    row_in[...] = jnp.zeros_like(row_in)
    col_in[...] = jnp.zeros_like(col_in)
    cor_in[...] = jnp.zeros_like(cor_in)
    for di, dj in DIRS:
        greet(di, dj)
    hs[...] = jnp.zeros_like(hs)
    rh[...] = jnp.zeros_like(rh)
    n_peers = sum(there(di, dj).astype(jnp.int32) for di, dj in DIRS)
    pl.semaphore_wait(barrier, n_peers)
    moves = [(-1, 0, 0), (1, 0, 0)] + [(di, dj, 0) for di in (-1, 1) for dj in (-1, 1)]
    bounds = ((0, RIM), (RIM, n_pairs - RIM), (n_pairs - RIM, n_pairs))
    moves += [(0, dj, g) for g in range(3) for dj in (-1, 1)]
    rim = (0, 1, 2, 3, 4, 5, 6, 7, 10, 11)
    middle = (8, 9)

    def landing(m, par):
        di, dj, g = moves[m]
        if di == 0:
            return col_in.at[par, (dj + 1) // 2, pl.ds(bounds[g][0], bounds[g][1] - bounds[g][0])]
        return row_in.at[par, (di + 1) // 2] if dj == 0 else cor_in.at[par, m - 2]

    def move(m, par):
        di, dj, g = moves[m]
        cols = {-1: pl.ds(MARGIN, halo), 1: pl.ds(MARGIN + width - halo, halo), 0: pl.ds(MARGIN, width)}[dj]
        if di == 0:
            rows = pl.ds(first + bounds[g][0], bounds[g][1] - bounds[g][0])
        else:
            rows = pl.ds(first if di < 0 else first + n_pairs - k, k)
        return pltpu.make_async_remote_copy(
            src_ref=hs.at[rows, cols, :], dst_ref=landing(m, par), send_sem=send_sem.at[m], recv_sem=recv_sem.at[par, m],
            device_id=device(di, dj), device_id_type=pl.DeviceIdType.LOGICAL)

    def send(which, par):
        for m in which:
            @pl.when(there(moves[m][0], moves[m][1]))
            def _():
                move(m, par).start()

    def receive(which, par):
        for m in which:
            @pl.when(there(-moves[m][0], -moves[m][1]))
            def _():
                move(m, par).wait_recv()
        for m in which:
            di, dj, g = moves[m]
            cols = {-1: pl.ds(MARGIN + width, halo), 1: pl.ds(MARGIN - halo, halo), 0: pl.ds(MARGIN, width)}[dj]
            if di == 0:
                rows = pl.ds(first + bounds[g][0], bounds[g][1] - bounds[g][0])
            else:
                rows = pl.ds(first + n_pairs if di < 0 else first - k, k)
            hs[rows, cols, :] = landing(m, par)[...]

    lane = lax.broadcasted_iota(jnp.int32, (1, 1, 128), 2)
    low = lane < 64

    def conv_zr(q0, n):
        parts = []
        for c in range(3):
            cols = pl.ds(MARGIN - 9 + c, COMP)
            own = hs[q0:q0 + n, cols, :]
            edge = jnp.where(low, hs[q0 + 1:q0 + 1 + n, cols, :], hs[q0 - 1:q0 - 1 + n, cols, :])
            parts += [own.astype(jnp.bfloat16), edge.astype(jnp.bfloat16)]
        lhs = jnp.concatenate(parts, axis=-1).reshape(n * COMP, 6 * 128)
        return jnp.dot(lhs, wzr_ref[...], preferred_element_type=jnp.float32)

    def conv_n(q0, n):
        parts = []
        for c in range(3):
            cols = pl.ds(MARGIN - 9 + c, COMP)
            own = rh[q0:q0 + n, cols, :].astype(jnp.bfloat16).reshape(n // 2, 2, COMP, 128)
            edge = jnp.stack([jnp.where(low[0], rh[q + 2, cols, :], rh[q - 1, cols, :]).astype(jnp.bfloat16) for q in range(q0, q0 + n, 2)])
            parts += [own[:, 0], own[:, 1], edge]
        lhs = jnp.concatenate(parts, axis=-1).reshape(n // 2 * COMP, 9 * 128)
        return jnp.dot(lhs, wn_ref[...], preferred_element_type=jnp.float32)

    def sigmoid(v):
        return 0.5 * jnp.tanh(0.5 * v) + 0.5

    in_top, in_bottom = my_row > 0, my_row < n_rows - 1
    in_left, in_right = my_col > 0, my_col < n_cols - 1

    def zr_chunk(s, q0, n):
        acc = conv_zr(q0, n) + gate_zr[s, q0 - 1:q0 - 1 + n].reshape(n * COMP, 256)
        z = sigmoid(acc[:, :128])
        r = sigmoid(acc[:, 128:])
        zs[q0:q0 + n] = z.reshape(n, COMP, 128)
        rh[q0:q0 + n, MARGIN - 8:MARGIN - 8 + COMP, :] = r.reshape(n, COMP, 128) * hs[q0:q0 + n, MARGIN - 8:MARGIN - 8 + COMP, :]

    def n_chunk(s, q0, n, t, last):
        g0 = (q0 - first + k - 1 - s) // 2
        acc = conv_n(q0, n) + gate_n[s, g0:g0 + n // 2].reshape(n // 2 * COMP, 256)
        both = jnp.tanh(acc).reshape(n // 2, COMP, 256)
        cand = jnp.stack([both[:, :, :128], both[:, :, 128:]], axis=1).reshape(n, COMP, 128)
        h = hs[q0:q0 + n, MARGIN - 8:MARGIN - 8 + COMP, :]
        h_new = cand + zs[q0:q0 + n] * (h - cand)
        inner = h_new[:, 8:8 + width, :]
        for i in range(n):
            q = q0 + i - first
            keep = in_top if q < 0 else in_bottom if q >= n_pairs else None
            at = pl.ds(MARGIN, width)
            hs[q0 + i, at, :] = inner[i] if keep is None else jnp.where(keep, inner[i], 0.0)
            if not last:
                for lo, inside in ((0, in_left), (8 + width, in_right)):
                    inside = inside if keep is None else jnp.logical_and(inside, keep)
                    hs[q0 + i, MARGIN - 8 + lo:MARGIN + lo, :] = jnp.where(inside, h_new[i, lo:lo + 8, :], 0.0)
            if 0 <= q < n_pairs:
                seq_ref[t, q] = inner[i].T.astype(jnp.bfloat16)

    def chunks(lo, hi, size):
        for q0 in range(lo, hi, size):
            yield q0, min(size, hi - q0)

    n_sub = x_ref.shape[1]
    edge = halo * 8
    lane2 = lax.broadcasted_iota(jnp.int32, (1, 128), 1)

    def wide(v):
        return jnp.concatenate([v, jnp.zeros((v.shape[0], 128 - v.shape[1]), v.dtype)], axis=1)

    def x_copy(d):
        di, dj = DIRS[d]
        if dj == 0:
            src = x_ref.at[:, pl.ds(0 if di < 0 else n_sub - edge, edge), :]
            dst = x_row_in.at[0 if di < 0 else 1]
        else:
            rows = {-1: pl.ds(0, edge), 1: pl.ds(n_sub - edge, edge), 0: pl.ds(0, n_sub)}[di]
            there_rows = {-1: pl.ds(edge + n_sub, edge), 1: pl.ds(0, edge), 0: pl.ds(edge, n_sub)}[di]
            side = 0 if dj < 0 else 1
            src = x_pack.at[side, rows, :]
            dst = x_col_in.at[side, there_rows, :]
        return pltpu.make_async_remote_copy(
            src_ref=src, dst_ref=dst, send_sem=x_send_sem.at[d], recv_sem=x_recv_sem.at[d],
            device_id=device(di, dj), device_id_type=pl.DeviceIdType.LOGICAL)

    def pack_x():
        for side in range(2):
            packed = jnp.zeros((n_sub, 128), jnp.float32)
            for t in range(n_steps):
                x = wide(x_ref[t].astype(jnp.float32))
                here = jnp.logical_and(lane2 >= 8 * t, lane2 < 8 * t + 8)
                packed = jnp.where(here, pltpu.roll(x, (8 * t - side * (width - 8)) % 128, 1), packed)
            x_pack[side] = packed.astype(jnp.bfloat16)

    def build_x(t, s):
        lo = lane2 < 8
        hi = lane2 >= 8 + width
        for first_sub, n, own, col in ((8, edge, x_row_in[1, t], 0), (8 + edge, n_sub, x_ref[t], edge), (8 + edge + n_sub, edge, x_row_in[0, t], edge + n_sub)):
            v = pltpu.roll(wide(own.astype(jnp.float32)), 8, 1)
            from_left = pltpu.roll(x_col_in[1, col:col + n, :].astype(jnp.float32), lax.rem(128 - 8 * t, 128), 1)
            from_right = pltpu.roll(x_col_in[0, col:col + n, :].astype(jnp.float32), lax.rem(128 + 8 + width - 8 * t, 128), 1)
            v = jnp.where(lo, from_left, jnp.where(hi, from_right, v))
            xs[0, first_sub:first_sub + n, :] = pltpu.roll(v, 1, 1)
            xs[1, first_sub:first_sub + n, :] = v
            xs[2, first_sub:first_sub + n, :] = pltpu.roll(v, 127, 1)
        zero = jnp.zeros((32, 128), jnp.bfloat16)
        for i in range(n_pairs + 2 * k):
            both = jnp.concatenate([xs[c, 16 * i:16 * i + 32].astype(jnp.bfloat16) for c in range(3)] + [zero], axis=0)
            xl[i] = both.T[:COMP]
        ext = k - 1 - s
        bias_zr = jnp.concatenate([b_ref[0:1, :], b_ref[1:2, :]], axis=1)
        bias_n = jnp.concatenate([b_ref[2:3, :], b_ref[2:3, :]], axis=1)
        for i, n in chunks(k - ext - 1, k + n_pairs + ext + 1, 2):
            part = jnp.dot(xl[i:i + n].reshape(n * COMP, 128), wxzr_ref[...], preferred_element_type=jnp.float32)
            gate_zr[s, i:i + n] = (part + bias_zr).reshape(n, COMP, 256)
        for g0, n in chunks(0, n_pairs // 2 + ext, 2):
            i = k - ext + 2 * g0
            two = xl[i:i + 2 * n].reshape(n, 2, COMP, 128)
            lhs = jnp.concatenate([two[:, 0], two[:, 1]], axis=-1).reshape(n * COMP, 256)
            part = jnp.dot(lhs, wxn_ref[...], preferred_element_type=jnp.float32)
            gate_n[s, g0:g0 + n] = (part + bias_n).reshape(n, COMP, 256)

    def fold_weights():
        def pair(get, a0, a1, gate):
            lo_part = get(a0, gate, 0) if 0 <= a0 <= 2 else None
            hi_part = get(a1, gate, 1) if 0 <= a1 <= 2 else None
            zero = jnp.zeros_like(lo_part if hi_part is None else hi_part)
            return jnp.where(lane2 < 64, zero if lo_part is None else lo_part, zero if hi_part is None else hi_part)

        for c in range(3):
            def get_h(a, gate, high):
                if gate == 2:
                    v = wide(whn_raw[a, c].astype(jnp.float32))
                    return pltpu.roll(v, 64, 1) if high else v
                v = whzr_raw[a, c].astype(jnp.float32)
                return pltpu.roll(v, 64, 1) if high != gate else v

            def get_x(a, gate, high):
                v = wx_raw[a, c].astype(jnp.float32)
                v = wide(v[:, 128:]) if gate == 2 else v[:, :128]
                return pltpu.roll(v, 64, 1) if high != (gate % 2) else v

            for j, rho in enumerate((0, 1, 2, -1)):
                at = c * 256 + j * 64
                for gate in range(2):
                    wzr_ref[at:at + 64, gate * 128:gate * 128 + 128] = pair(get_h, rho + 1, rho, gate).astype(jnp.bfloat16)
            for j, rho in enumerate((0, 1, 2, 3, 4, -1)):
                at = c * 384 + j * 64
                for o in (0, 2):
                    block = pair(get_h, rho - o + 1, rho - o, 2) if -1 <= rho - o <= 2 else jnp.zeros((64, 128), jnp.float32)
                    wn_ref[at:at + 64, o * 64:o * 64 + 128] = block.astype(jnp.bfloat16)
            for j, rho in enumerate((-1, 0, 1, 2)):
                at = c * 32 + j * 8
                for gate in range(3):
                    wx_ref[at:at + 8, gate * 128:gate * 128 + 128] = pair(get_x, rho + 1, rho, gate)
        wx_ref[96:128, :] = jnp.zeros((32, 384), jnp.float32)
        wxzr_ref[...] = wx_ref[:, :256].astype(jnp.bfloat16)
        wxn_ref[...] = jnp.zeros_like(wxn_ref)
        wxn_ref[0:128, 0:128] = wx_ref[:, 256:].astype(jnp.bfloat16)
        wxn_ref[128:256, 128:256] = wx_ref[:, 256:].astype(jnp.bfloat16)
        zr = bias_raw[:, :128]
        turned = pltpu.roll(zr, 64, 1)
        cand = wide(bias_raw[:, 128:])
        b_ref[0:1, :] = jnp.where(lane2 < 64, zr, turned)
        b_ref[1:2, :] = jnp.where(lane2 < 64, turned, zr)
        b_ref[2:3, :] = jnp.where(lane2 < 64, cand, pltpu.roll(cand, 64, 1))

    loads[0].wait()
    pack_x()
    for d, (di, dj) in enumerate(DIRS):
        @pl.when(there(di, dj))
        def _():
            x_copy(d).start()
    loads[1].wait()
    for q in range(n_pairs):
        hs[first + q, MARGIN:MARGIN + width, :] = h_ref[q].T
    send(rim, 0)
    send(middle, 0)
    for load in loads[2:]:
        load.wait()
    fold_weights()
    xs[...] = jnp.zeros_like(xs)
    for d, (di, dj) in enumerate(DIRS):
        @pl.when(there(-di, -dj))
        def _():
            x_copy(d).wait_recv()

    def zr(s, lo, hi):
        for q0, n in chunks(first + lo, first + hi, CHUNK):
            zr_chunk(s, q0, n)

    def cand(t, s, lo, hi):
        for q0, n in chunks(first + lo, first + hi, N_CHUNK):
            n_chunk(s, q0, n, t, s == k - 1)

    n_periods = n_steps // k

    def period(p, carry):
        par = lax.rem(p, 2)
        for s in range(k):
            build_x(p * k + s, s)
        for s in range(k):
            ext = k - 1 - s
            t = p * k + s
            if s == 0:
                receive(rim, par)
                zr(s, -ext - 1, RIM - 1)
                zr(s, n_pairs - RIM + 1, n_pairs + ext + 1)
                receive(middle, par)
                zr(s, RIM - 1, n_pairs - RIM + 1)
                for m, (di, dj, _) in enumerate(moves):
                    @pl.when(there(di, dj))
                    def _():
                        move(m, par).wait_send()
            if s < k - 1:
                if s > 0:
                    zr(s, -ext - 1, n_pairs + ext + 1)
                cand(t, s, -ext, n_pairs + ext)
            else:
                more = p + 1 < n_periods

                def send_next(which):
                    @pl.when(more)
                    def _():
                        send(which, 1 - par)
                if s > 0:
                    zr(s, -1, RIM + 1)
                    zr(s, n_pairs - RIM - 1, n_pairs + 1)
                cand(t, s, 0, RIM)
                cand(t, s, n_pairs - RIM, n_pairs)
                send_next(rim)
                if s > 0:
                    zr(s, RIM + 1, n_pairs - RIM - 1)
                cand(t, s, RIM, n_pairs - RIM)
                send_next(middle)
        return carry

    lax.fori_loop(0, n_steps // k, period, 0)
    for q in range(n_pairs):
        last_ref[q] = hs[first + q, MARGIN:MARGIN + width, :].T
    for d, (di, dj) in enumerate(DIRS):
        @pl.when(there(di, dj))
        def _():
            x_copy(d).wait_send()


def solution(mesh):
    n_rows = mesh.shape['rows']
    n_cols = mesh.shape['cols']
    frame_spec = P(None, 'batch', 'rows', 'cols', None)
    state_spec = P('batch', 'rows', 'cols', None)

    def local_fn(frames, h_init, w_x, w_hzr, w_hn, gate_bias):
        n_steps, _, tile_h, width, c_in = frames.shape
        n_hidden = h_init.shape[-1]
        k = FUSE
        n_pairs = tile_h // 2
        x = frames[:, 0].transpose(0, 1, 3, 2).reshape(n_steps, tile_h * c_in, width)
        h0 = h_init[0].transpose(0, 2, 1).reshape(n_pairs, 2 * n_hidden, width)
        edge = 2 * k * c_in
        n_buf = n_pairs + 2 * k + 2
        vmem = pl.BlockSpec(memory_space=pltpu.VMEM)
        seq, last = pl.pallas_call(
            functools.partial(kernel, (n_steps, n_pairs, width, n_rows, n_cols)),
            out_shape=(pltpu.VMEM((n_steps, n_pairs, 128, width), jnp.bfloat16),
                       jax.ShapeDtypeStruct((n_pairs, 128, width), jnp.float32)),
            in_specs=[pl.BlockSpec(memory_space=pltpu.HBM)] * 6,
            out_specs=(vmem, vmem),
            scratch_shapes=[
                pltpu.VMEM(x.shape, x.dtype),
                pltpu.VMEM(h0.shape, h0.dtype),
                pltpu.VMEM(w_x.shape, w_x.dtype),
                pltpu.VMEM(w_hzr.shape, w_hzr.dtype),
                pltpu.VMEM(w_hn.shape, w_hn.dtype),
                pltpu.VMEM((1, gate_bias.shape[0]), gate_bias.dtype),
                pltpu.VMEM((n_buf, 128, 128), jnp.float32),
                pltpu.VMEM((n_buf, 128, 128), jnp.float32),
                pltpu.VMEM((n_buf, COMP, 128), jnp.float32),
                pltpu.VMEM((n_pairs + 2 * k, COMP, 128), jnp.bfloat16),
                pltpu.VMEM((k, n_pairs + 2 * k, COMP, 256), jnp.float32),
                pltpu.VMEM((k, n_pairs // 2 + k - 1, COMP, 256), jnp.float32),
                pltpu.VMEM((2, 2, k, width, 128), jnp.float32),
                pltpu.VMEM((2, 2, n_pairs, 2 * k, 128), jnp.float32),
                pltpu.VMEM((2, 4, k, 2 * k, 128), jnp.float32),
                pltpu.VMEM((768, 256), jnp.bfloat16),
                pltpu.VMEM((1152, 256), jnp.bfloat16),
                pltpu.VMEM((128, 384), jnp.float32),
                pltpu.VMEM((128, 256), jnp.bfloat16),
                pltpu.VMEM((256, 256), jnp.bfloat16),
                pltpu.VMEM((3, 128), jnp.float32),
                pltpu.VMEM((3, tile_h * c_in + 2 * edge + 16, 128), jnp.float32),
                pltpu.VMEM((2, tile_h * c_in, 128), jnp.bfloat16),
                pltpu.VMEM((2, n_steps, edge, width), jnp.bfloat16),
                pltpu.VMEM((2, tile_h * c_in + 2 * edge, 128), jnp.bfloat16),
                pltpu.SemaphoreType.DMA((12,)),
                pltpu.SemaphoreType.DMA((2, 12)),
                pltpu.SemaphoreType.DMA((8,)),
                pltpu.SemaphoreType.DMA((8,)),
                pltpu.SemaphoreType.DMA((6,)),
            ],
            compiler_params=pltpu.CompilerParams(collective_id=0, has_side_effects=True, vmem_limit_bytes=32 * 2**20),
        )(*[pltpu.with_memory_space_constraint(v, pltpu.HBM) for v in (x, h0, w_x, w_hzr, w_hn, gate_bias.reshape(1, -1))])
        seq = seq.reshape(n_steps, 1, tile_h, n_hidden, width).transpose(0, 1, 2, 4, 3)
        last = last.reshape(1, tile_h, n_hidden, width).transpose(0, 1, 3, 2)
        return seq, last

    return jax.shard_map(local_fn, mesh=mesh, in_specs=(frame_spec, state_spec, P(), P(), P(), P()), out_specs=(frame_spec, state_spec), check_vma=False)
```

```python
import functools

import jax
import jax.numpy as jnp
from jax import lax
from jax.experimental import pallas as pl
from jax.experimental.pallas import tpu as pltpu
from jax.sharding import PartitionSpec as P

FUSE = 4
CHUNK = 2
N_CHUNK = 2
MARGIN = 16
SUBLANES = 128
COMP = 112
DIRS = ((-1, 0), (1, 0), (0, -1), (0, 1), (-1, -1), (-1, 1), (1, -1), (1, 1))


def kernel(dims, x_hbm, h_hbm, wx_hbm, whzr_hbm, whn_hbm, bias_hbm, seq_ref, last_ref,
           x_ref, h_ref, wx_raw, whzr_raw, whn_raw, bias_raw,
           hs, rh, zs, xl, gate_zr, gate_n, row_in, col_in, cor_in, wzr_ref, wn_ref, wx_ref, wxzr_ref, wxn_ref, b_ref, xs, x_pack, x_row_in, x_col_in,
           send_sem, recv_sem, x_send_sem, x_recv_sem, load_sem):
    n_steps, n_pairs, width, n_rows, n_cols = dims
    k = FUSE
    halo = 2 * k
    first = k + 1
    my_row = lax.axis_index('rows')
    my_col = lax.axis_index('cols')

    def there(di, dj):
        r, c = my_row + di, my_col + dj
        return jnp.logical_and(jnp.logical_and(r >= 0, r < n_rows), jnp.logical_and(c >= 0, c < n_cols))

    loads = [pltpu.make_async_copy(src, dst, load_sem.at[i]) for i, (src, dst) in enumerate(
        ((x_hbm, x_ref), (h_hbm, h_ref), (wx_hbm, wx_raw), (whzr_hbm, whzr_raw), (whn_hbm, whn_raw), (bias_hbm, bias_raw)))]
    for load in loads:
        load.start()
    barrier = pltpu.get_barrier_semaphore()
    def device(di, dj):
        return (lax.axis_index('batch') * n_cols + my_col + dj) * n_rows + my_row + di

    def greet(di, dj):
        @pl.when(there(di, dj))
        def _():
            pl.semaphore_signal(barrier, inc=1, device_id=device(di, dj),
                                device_id_type=pl.DeviceIdType.LOGICAL)

    x_row_in[...] = jnp.zeros_like(x_row_in)
    x_col_in[...] = jnp.zeros_like(x_col_in)
    row_in[...] = jnp.zeros_like(row_in)
    col_in[...] = jnp.zeros_like(col_in)
    cor_in[...] = jnp.zeros_like(cor_in)
    for di, dj in DIRS:
        greet(di, dj)
    hs[...] = jnp.zeros_like(hs)
    rh[...] = jnp.zeros_like(rh)
    n_peers = sum(there(di, dj).astype(jnp.int32) for di, dj in DIRS)
    moves = [(-1, 0), (1, 0)] + [(di, dj) for di in (-1, 1) for dj in (-1, 1)]
    moves += [(0, -1), (0, 1)]
    order = (2, 3, 4, 5, 6, 7, 0, 1)

    def landing(m, par):
        di, dj = moves[m]
        if di == 0:
            return col_in.at[par, (dj + 1) // 2]
        return row_in.at[par, (di + 1) // 2] if dj == 0 else cor_in.at[par, m - 2]

    def move(m, par):
        di, dj = moves[m]
        cols = {-1: pl.ds(MARGIN, halo), 1: pl.ds(MARGIN + width - halo, halo), 0: pl.ds(MARGIN, width)}[dj]
        if di == 0:
            rows = pl.ds(first, n_pairs)
        else:
            rows = pl.ds(first if di < 0 else first + n_pairs - k, k)
        return pltpu.make_async_remote_copy(
            src_ref=hs.at[rows, cols, :], dst_ref=landing(m, par), send_sem=send_sem.at[m], recv_sem=recv_sem.at[par, m],
            device_id=device(di, dj), device_id_type=pl.DeviceIdType.LOGICAL)

    def send(par):
        for m in order:
            @pl.when(there(moves[m][0], moves[m][1]))
            def _():
                move(m, par).start()

    def receive(par):
        for m in order:
            @pl.when(there(-moves[m][0], -moves[m][1]))
            def _():
                move(m, par).wait_recv()
        for m in order:
            di, dj = moves[m]
            cols = {-1: pl.ds(MARGIN + width, halo), 1: pl.ds(MARGIN - halo, halo), 0: pl.ds(MARGIN, width)}[dj]
            if di == 0:
                rows = pl.ds(first, n_pairs)
            else:
                rows = pl.ds(first + n_pairs if di < 0 else first - k, k)
            hs[rows, cols, :] = landing(m, par)[...]

    lane = lax.broadcasted_iota(jnp.int32, (1, 1, 128), 2)
    low = lane < 64

    def conv_zr(q0, n):
        parts = []
        for c in range(3):
            cols = pl.ds(MARGIN - 9 + c, COMP)
            own = hs[q0:q0 + n, cols, :]
            edge = jnp.where(low, hs[q0 + 1:q0 + 1 + n, cols, :], hs[q0 - 1:q0 - 1 + n, cols, :])
            parts += [own.astype(jnp.bfloat16), edge.astype(jnp.bfloat16)]
        lhs = jnp.concatenate(parts, axis=-1).reshape(n * COMP, 6 * 128)
        return jnp.dot(lhs, wzr_ref[...], preferred_element_type=jnp.float32)

    def conv_n(q0, n):
        parts = []
        for c in range(3):
            cols = pl.ds(MARGIN - 9 + c, COMP)
            own = rh[q0:q0 + n, cols, :].astype(jnp.bfloat16).reshape(n // 2, 2, COMP, 128)
            edge = jnp.stack([jnp.where(low[0], rh[q + 2, cols, :], rh[q - 1, cols, :]).astype(jnp.bfloat16) for q in range(q0, q0 + n, 2)])
            parts += [own[:, 0], own[:, 1], edge]
        lhs = jnp.concatenate(parts, axis=-1).reshape(n // 2 * COMP, 9 * 128)
        return jnp.dot(lhs, wn_ref[...], preferred_element_type=jnp.float32)

    def sigmoid(v):
        return 0.5 * jnp.tanh(0.5 * v) + 0.5

    in_top, in_bottom = my_row > 0, my_row < n_rows - 1
    in_left, in_right = my_col > 0, my_col < n_cols - 1

    def zr_chunk(s, q0, n):
        acc = conv_zr(q0, n) + gate_zr[s, q0 - 1:q0 - 1 + n].reshape(n * COMP, 256)
        z = sigmoid(acc[:, :128])
        r = sigmoid(acc[:, 128:])
        zs[q0:q0 + n] = z.reshape(n, COMP, 128)
        rh[q0:q0 + n, MARGIN - 8:MARGIN - 8 + COMP, :] = r.reshape(n, COMP, 128) * hs[q0:q0 + n, MARGIN - 8:MARGIN - 8 + COMP, :]

    def n_chunk(s, q0, n, t, last):
        g0 = (q0 - first + k - 1 - s) // 2
        acc = conv_n(q0, n) + gate_n[s, g0:g0 + n // 2].reshape(n // 2 * COMP, 256)
        both = jnp.tanh(acc).reshape(n // 2, COMP, 256)
        cand = jnp.stack([both[:, :, :128], both[:, :, 128:]], axis=1).reshape(n, COMP, 128)
        h = hs[q0:q0 + n, MARGIN - 8:MARGIN - 8 + COMP, :]
        h_new = cand + zs[q0:q0 + n] * (h - cand)
        inner = h_new[:, 8:8 + width, :]
        for i in range(n):
            q = q0 + i - first
            keep = in_top if q < 0 else in_bottom if q >= n_pairs else None
            at = pl.ds(MARGIN, width)
            hs[q0 + i, at, :] = inner[i] if keep is None else jnp.where(keep, inner[i], 0.0)
            if not last:
                for lo, inside in ((0, in_left), (8 + width, in_right)):
                    inside = inside if keep is None else jnp.logical_and(inside, keep)
                    hs[q0 + i, MARGIN - 8 + lo:MARGIN + lo, :] = jnp.where(inside, h_new[i, lo:lo + 8, :], 0.0)
            if 0 <= q < n_pairs:
                seq_ref[t, q] = inner[i].T.astype(jnp.bfloat16)

    def chunks(lo, hi, size):
        for q0 in range(lo, hi, size):
            yield q0, min(size, hi - q0)

    n_sub = x_ref.shape[1]
    edge = halo * 8
    lane2 = lax.broadcasted_iota(jnp.int32, (1, 128), 1)

    def wide(v):
        return jnp.concatenate([v, jnp.zeros((v.shape[0], 128 - v.shape[1]), v.dtype)], axis=1)

    def x_copy(d):
        di, dj = DIRS[d]
        if dj == 0:
            src = x_ref.at[:, pl.ds(0 if di < 0 else n_sub - edge, edge), :]
            dst = x_row_in.at[0 if di < 0 else 1]
        else:
            rows = {-1: pl.ds(0, edge), 1: pl.ds(n_sub - edge, edge), 0: pl.ds(0, n_sub)}[di]
            there_rows = {-1: pl.ds(edge + n_sub, edge), 1: pl.ds(0, edge), 0: pl.ds(edge, n_sub)}[di]
            side = 0 if dj < 0 else 1
            src = x_pack.at[side, rows, :]
            dst = x_col_in.at[side, there_rows, :]
        return pltpu.make_async_remote_copy(
            src_ref=src, dst_ref=dst, send_sem=x_send_sem.at[d], recv_sem=x_recv_sem.at[d],
            device_id=device(di, dj), device_id_type=pl.DeviceIdType.LOGICAL)

    def pack_x():
        for side in range(2):
            packed = jnp.zeros((n_sub, 128), jnp.float32)
            for t in range(n_steps):
                x = wide(x_ref[t].astype(jnp.float32))
                here = jnp.logical_and(lane2 >= 8 * t, lane2 < 8 * t + 8)
                packed = jnp.where(here, pltpu.roll(x, (8 * t - side * (width - 8)) % 128, 1), packed)
            x_pack[side] = packed.astype(jnp.bfloat16)

    def build_x(t, s):
        lo = lane2 < 8
        hi = lane2 >= 8 + width
        for first_sub, n, own, col in ((8, edge, x_row_in[1, t], 0), (8 + edge, n_sub, x_ref[t], edge), (8 + edge + n_sub, edge, x_row_in[0, t], edge + n_sub)):
            v = pltpu.roll(wide(own.astype(jnp.float32)), 8, 1)
            from_left = pltpu.roll(x_col_in[1, col:col + n, :].astype(jnp.float32), lax.rem(128 - 8 * t, 128), 1)
            from_right = pltpu.roll(x_col_in[0, col:col + n, :].astype(jnp.float32), lax.rem(128 + 8 + width - 8 * t, 128), 1)
            v = jnp.where(lo, from_left, jnp.where(hi, from_right, v))
            xs[0, first_sub:first_sub + n, :] = pltpu.roll(v, 1, 1)
            xs[1, first_sub:first_sub + n, :] = v
            xs[2, first_sub:first_sub + n, :] = pltpu.roll(v, 127, 1)
        zero = jnp.zeros((32, 128), jnp.bfloat16)
        for i in range(n_pairs + 2 * k):
            both = jnp.concatenate([xs[c, 16 * i:16 * i + 32].astype(jnp.bfloat16) for c in range(3)] + [zero], axis=0)
            xl[i] = both.T[:COMP]
        ext = k - 1 - s
        bias_zr = jnp.concatenate([b_ref[0:1, :], b_ref[1:2, :]], axis=1)
        bias_n = jnp.concatenate([b_ref[2:3, :], b_ref[2:3, :]], axis=1)
        for i, n in chunks(k - ext - 1, k + n_pairs + ext + 1, 2):
            part = jnp.dot(xl[i:i + n].reshape(n * COMP, 128), wxzr_ref[...], preferred_element_type=jnp.float32)
            gate_zr[s, i:i + n] = (part + bias_zr).reshape(n, COMP, 256)
        for g0, n in chunks(0, n_pairs // 2 + ext, 2):
            i = k - ext + 2 * g0
            two = xl[i:i + 2 * n].reshape(n, 2, COMP, 128)
            lhs = jnp.concatenate([two[:, 0], two[:, 1]], axis=-1).reshape(n * COMP, 256)
            part = jnp.dot(lhs, wxn_ref[...], preferred_element_type=jnp.float32)
            gate_n[s, g0:g0 + n] = (part + bias_n).reshape(n, COMP, 256)

    def fold_weights():
        def pair(get, a0, a1, gate):
            lo_part = get(a0, gate, 0) if 0 <= a0 <= 2 else None
            hi_part = get(a1, gate, 1) if 0 <= a1 <= 2 else None
            zero = jnp.zeros_like(lo_part if hi_part is None else hi_part)
            return jnp.where(lane2 < 64, zero if lo_part is None else lo_part, zero if hi_part is None else hi_part)

        for c in range(3):
            def get_h(a, gate, high):
                if gate == 2:
                    v = wide(whn_raw[a, c].astype(jnp.float32))
                    return pltpu.roll(v, 64, 1) if high else v
                v = whzr_raw[a, c].astype(jnp.float32)
                return pltpu.roll(v, 64, 1) if high != gate else v

            def get_x(a, gate, high):
                v = wx_raw[a, c].astype(jnp.float32)
                v = wide(v[:, 128:]) if gate == 2 else v[:, :128]
                return pltpu.roll(v, 64, 1) if high != (gate % 2) else v

            for j, rho in enumerate((0, 1, 2, -1)):
                at = c * 256 + j * 64
                for gate in range(2):
                    wzr_ref[at:at + 64, gate * 128:gate * 128 + 128] = pair(get_h, rho + 1, rho, gate).astype(jnp.bfloat16)
            for j, rho in enumerate((0, 1, 2, 3, 4, -1)):
                at = c * 384 + j * 64
                for o in (0, 2):
                    block = pair(get_h, rho - o + 1, rho - o, 2) if -1 <= rho - o <= 2 else jnp.zeros((64, 128), jnp.float32)
                    wn_ref[at:at + 64, o * 64:o * 64 + 128] = block.astype(jnp.bfloat16)
            for j, rho in enumerate((-1, 0, 1, 2)):
                at = c * 32 + j * 8
                for gate in range(3):
                    wx_ref[at:at + 8, gate * 128:gate * 128 + 128] = pair(get_x, rho + 1, rho, gate)
        wx_ref[96:128, :] = jnp.zeros((32, 384), jnp.float32)
        wxzr_ref[...] = wx_ref[:, :256].astype(jnp.bfloat16)
        wxn_ref[...] = jnp.zeros_like(wxn_ref)
        wxn_ref[0:128, 0:128] = wx_ref[:, 256:].astype(jnp.bfloat16)
        wxn_ref[128:256, 128:256] = wx_ref[:, 256:].astype(jnp.bfloat16)
        zr = bias_raw[:, :128]
        turned = pltpu.roll(zr, 64, 1)
        cand = wide(bias_raw[:, 128:])
        b_ref[0:1, :] = jnp.where(lane2 < 64, zr, turned)
        b_ref[1:2, :] = jnp.where(lane2 < 64, turned, zr)
        b_ref[2:3, :] = jnp.where(lane2 < 64, cand, pltpu.roll(cand, 64, 1))

    loads[0].wait()
    pack_x()
    pl.semaphore_wait(barrier, n_peers)
    for d, (di, dj) in enumerate(DIRS):
        @pl.when(there(di, dj))
        def _():
            x_copy(d).start()
    loads[1].wait()
    for q in range(n_pairs):
        hs[first + q, MARGIN:MARGIN + width, :] = h_ref[q].T
    send(0)
    for load in loads[2:]:
        load.wait()
    fold_weights()
    xs[...] = jnp.zeros_like(xs)
    for d, (di, dj) in enumerate(DIRS):
        @pl.when(there(-di, -dj))
        def _():
            x_copy(d).wait_recv()

    def zr(s, lo, hi):
        for q0, n in chunks(first + lo, first + hi, CHUNK):
            zr_chunk(s, q0, n)

    def cand(t, s, lo, hi):
        for q0, n in chunks(first + lo, first + hi, N_CHUNK):
            n_chunk(s, q0, n, t, s == k - 1)

    n_periods = n_steps // k

    def period(p, carry):
        par = lax.rem(p, 2)
        for s in range(k):
            build_x(p * k + s, s)
        for s in range(k):
            ext = k - 1 - s
            t = p * k + s
            if s == 0:
                receive(par)
                for m, (di, dj) in enumerate(moves):
                    @pl.when(there(di, dj))
                    def _():
                        move(m, par).wait_send()
                zr(s, -ext - 1, n_pairs + ext + 1)
            if s < k - 1:
                if s > 0:
                    zr(s, -ext - 1, n_pairs + ext + 1)
                cand(t, s, -ext, n_pairs + ext)
            else:
                more = p + 1 < n_periods

                if s > 0:
                    zr(s, -1, n_pairs + 1)
                cand(t, s, 0, n_pairs)

                @pl.when(more)
                def _():
                    send(1 - par)
        return carry

    lax.fori_loop(0, n_steps // k, period, 0)
    for q in range(n_pairs):
        last_ref[q] = hs[first + q, MARGIN:MARGIN + width, :].T
    for d, (di, dj) in enumerate(DIRS):
        @pl.when(there(di, dj))
        def _():
            x_copy(d).wait_send()


def solution(mesh):
    n_rows = mesh.shape['rows']
    n_cols = mesh.shape['cols']
    frame_spec = P(None, 'batch', 'rows', 'cols', None)
    state_spec = P('batch', 'rows', 'cols', None)

    def local_fn(frames, h_init, w_x, w_hzr, w_hn, gate_bias):
        n_steps, _, tile_h, width, c_in = frames.shape
        n_hidden = h_init.shape[-1]
        k = FUSE
        n_pairs = tile_h // 2
        x = frames[:, 0].transpose(0, 1, 3, 2).reshape(n_steps, tile_h * c_in, width)
        h0 = h_init[0].transpose(0, 2, 1).reshape(n_pairs, 2 * n_hidden, width)
        edge = 2 * k * c_in
        n_buf = n_pairs + 2 * k + 2
        vmem = pl.BlockSpec(memory_space=pltpu.VMEM)
        seq, last = pl.pallas_call(
            functools.partial(kernel, (n_steps, n_pairs, width, n_rows, n_cols)),
            out_shape=(pltpu.VMEM((n_steps, n_pairs, 128, width), jnp.bfloat16),
                       jax.ShapeDtypeStruct((n_pairs, 128, width), jnp.float32)),
            in_specs=[pl.BlockSpec(memory_space=pltpu.HBM)] * 6,
            out_specs=(vmem, vmem),
            scratch_shapes=[
                pltpu.VMEM(x.shape, x.dtype),
                pltpu.VMEM(h0.shape, h0.dtype),
                pltpu.VMEM(w_x.shape, w_x.dtype),
                pltpu.VMEM(w_hzr.shape, w_hzr.dtype),
                pltpu.VMEM(w_hn.shape, w_hn.dtype),
                pltpu.VMEM((1, gate_bias.shape[0]), gate_bias.dtype),
                pltpu.VMEM((n_buf, SUBLANES, 128), jnp.float32),
                pltpu.VMEM((n_buf, SUBLANES, 128), jnp.float32),
                pltpu.VMEM((n_buf, COMP, 128), jnp.float32),
                pltpu.VMEM((n_pairs + 2 * k, COMP, 128), jnp.bfloat16),
                pltpu.VMEM((k, n_pairs + 2 * k, COMP, 256), jnp.float32),
                pltpu.VMEM((k, n_pairs // 2 + k - 1, COMP, 256), jnp.float32),
                pltpu.VMEM((2, 2, k, width, 128), jnp.float32),
                pltpu.VMEM((2, 2, n_pairs, 2 * k, 128), jnp.float32),
                pltpu.VMEM((2, 4, k, 2 * k, 128), jnp.float32),
                pltpu.VMEM((768, 256), jnp.bfloat16),
                pltpu.VMEM((1152, 256), jnp.bfloat16),
                pltpu.VMEM((128, 384), jnp.float32),
                pltpu.VMEM((128, 256), jnp.bfloat16),
                pltpu.VMEM((256, 256), jnp.bfloat16),
                pltpu.VMEM((3, 128), jnp.float32),
                pltpu.VMEM((3, tile_h * c_in + 2 * edge + 16, 128), jnp.float32),
                pltpu.VMEM((2, tile_h * c_in, 128), jnp.bfloat16),
                pltpu.VMEM((2, n_steps, edge, width), jnp.bfloat16),
                pltpu.VMEM((2, tile_h * c_in + 2 * edge, 128), jnp.bfloat16),
                pltpu.SemaphoreType.DMA((8,)),
                pltpu.SemaphoreType.DMA((2, 8)),
                pltpu.SemaphoreType.DMA((8,)),
                pltpu.SemaphoreType.DMA((8,)),
                pltpu.SemaphoreType.DMA((6,)),
            ],
            compiler_params=pltpu.CompilerParams(collective_id=0, has_side_effects=True, vmem_limit_bytes=50 * 2**20),
        )(*[pltpu.with_memory_space_constraint(v, pltpu.HBM) for v in (x, h0, w_x, w_hzr, w_hn, gate_bias.reshape(1, -1))])
        seq = seq.reshape(n_steps, 1, tile_h, n_hidden, width).transpose(0, 1, 2, 4, 3)
        last = last.reshape(1, tile_h, n_hidden, width).transpose(0, 1, 3, 2)
        return seq, last

    return jax.shard_map(local_fn, mesh=mesh, in_specs=(frame_spec, state_spec, P(), P(), P(), P()), out_specs=(frame_spec, state_spec), check_vma=False)
```

```python
import functools

import jax
import jax.numpy as jnp
from jax import lax
from jax.experimental import pallas as pl
from jax.experimental.pallas import tpu as pltpu
from jax.sharding import PartitionSpec as P

FUSE = 4
CHUNK = 2
N_CHUNK = 4
MARGIN = 16
SUBLANES = 128
COMP = 112
DIRS = ((-1, 0), (1, 0), (0, -1), (0, 1), (-1, -1), (-1, 1), (1, -1), (1, 1))


def kernel(dims, x_hbm, h_hbm, wx_hbm, whzr_hbm, whn_hbm, bias_hbm, seq_ref, last_ref,
           x_ref, h_ref, wx_raw, whzr_raw, whn_raw, bias_raw,
           hs, rh, zs, xl, gate_zr, gate_n, row_in, col_in, cor_in, wzr_ref, wn_ref, wx_ref, wxzr_ref, wxn_ref, b_ref, xs, x_pack, x_row_in, x_col_in,
           send_sem, recv_sem, x_send_sem, x_recv_sem, load_sem):
    n_steps, n_pairs, width, n_rows, n_cols = dims
    k = FUSE
    halo = 2 * k
    first = k + 1
    my_row = lax.axis_index('rows')
    my_col = lax.axis_index('cols')

    def there(di, dj):
        r, c = my_row + di, my_col + dj
        return jnp.logical_and(jnp.logical_and(r >= 0, r < n_rows), jnp.logical_and(c >= 0, c < n_cols))

    loads = [pltpu.make_async_copy(src, dst, load_sem.at[i]) for i, (src, dst) in enumerate(
        ((x_hbm, x_ref), (h_hbm, h_ref), (wx_hbm, wx_raw), (whzr_hbm, whzr_raw), (whn_hbm, whn_raw), (bias_hbm, bias_raw)))]
    for load in loads:
        load.start()
    barrier = pltpu.get_barrier_semaphore()
    def device(di, dj):
        return (lax.axis_index('batch') * n_cols + my_col + dj) * n_rows + my_row + di

    def greet(di, dj):
        @pl.when(there(di, dj))
        def _():
            pl.semaphore_signal(barrier, inc=1, device_id=device(di, dj),
                                device_id_type=pl.DeviceIdType.LOGICAL)

    x_row_in[...] = jnp.zeros_like(x_row_in)
    x_col_in[...] = jnp.zeros_like(x_col_in)
    row_in[...] = jnp.zeros_like(row_in)
    col_in[...] = jnp.zeros_like(col_in)
    cor_in[...] = jnp.zeros_like(cor_in)
    for di, dj in DIRS:
        greet(di, dj)
    hs[...] = jnp.zeros_like(hs)
    rh[...] = jnp.zeros_like(rh)
    n_peers = sum(there(di, dj).astype(jnp.int32) for di, dj in DIRS)
    moves = [(-1, 0), (1, 0)] + [(di, dj) for di in (-1, 1) for dj in (-1, 1)]
    moves += [(0, -1), (0, 1)]
    order = (2, 3, 4, 5, 6, 7, 0, 1)

    def landing(m, par):
        di, dj = moves[m]
        if di == 0:
            return col_in.at[par, (dj + 1) // 2]
        return row_in.at[par, (di + 1) // 2] if dj == 0 else cor_in.at[par, m - 2]

    def move(m, par):
        di, dj = moves[m]
        cols = {-1: pl.ds(MARGIN, halo), 1: pl.ds(MARGIN + width - halo, halo), 0: pl.ds(MARGIN, width)}[dj]
        if di == 0:
            rows = pl.ds(first, n_pairs)
        else:
            rows = pl.ds(first if di < 0 else first + n_pairs - k, k)
        return pltpu.make_async_remote_copy(
            src_ref=hs.at[rows, cols, :], dst_ref=landing(m, par), send_sem=send_sem.at[m], recv_sem=recv_sem.at[par, m],
            device_id=device(di, dj), device_id_type=pl.DeviceIdType.LOGICAL)

    def send(par):
        for m in order:
            @pl.when(there(moves[m][0], moves[m][1]))
            def _():
                move(m, par).start()

    def receive(par):
        for m in order:
            @pl.when(there(-moves[m][0], -moves[m][1]))
            def _():
                move(m, par).wait_recv()
        for m in order:
            di, dj = moves[m]
            cols = {-1: pl.ds(MARGIN + width, halo), 1: pl.ds(MARGIN - halo, halo), 0: pl.ds(MARGIN, width)}[dj]
            if di == 0:
                rows = pl.ds(first, n_pairs)
            else:
                rows = pl.ds(first + n_pairs if di < 0 else first - k, k)
            hs[rows, cols, :] = landing(m, par)[...]

    lane = lax.broadcasted_iota(jnp.int32, (1, 1, 128), 2)
    low = lane < 64

    def conv_zr(q0, n):
        parts = []
        for c in range(3):
            cols = pl.ds(MARGIN - 9 + c, COMP)
            own = hs[q0:q0 + n, cols, :]
            edge = jnp.where(low, hs[q0 + 1:q0 + 1 + n, cols, :], hs[q0 - 1:q0 - 1 + n, cols, :])
            parts += [own.astype(jnp.bfloat16), edge.astype(jnp.bfloat16)]
        lhs = jnp.concatenate(parts, axis=-1).reshape(n * COMP, 6 * 128)
        return jnp.dot(lhs, wzr_ref[...], preferred_element_type=jnp.float32)

    def conv_n(q0, n):
        parts = []
        for c in range(3):
            cols = pl.ds(MARGIN - 9 + c, COMP)
            own = rh[q0:q0 + n, cols, :].astype(jnp.bfloat16).reshape(n // 2, 2, COMP, 128)
            edge = jnp.stack([jnp.where(low[0], rh[q + 2, cols, :], rh[q - 1, cols, :]).astype(jnp.bfloat16) for q in range(q0, q0 + n, 2)])
            parts += [own[:, 0], own[:, 1], edge]
        lhs = jnp.concatenate(parts, axis=-1).reshape(n // 2 * COMP, 9 * 128)
        return jnp.dot(lhs, wn_ref[...], preferred_element_type=jnp.float32)

    def sigmoid(v):
        return 0.5 * jnp.tanh(0.5 * v) + 0.5

    in_top, in_bottom = my_row > 0, my_row < n_rows - 1
    in_left, in_right = my_col > 0, my_col < n_cols - 1

    def zr_chunk(s, q0, n):
        acc = conv_zr(q0, n) + gate_zr[s, q0 - 1:q0 - 1 + n].reshape(n * COMP, 256)
        z = sigmoid(acc[:, :128])
        r = sigmoid(acc[:, 128:])
        zs[q0:q0 + n] = z.reshape(n, COMP, 128)
        rh[q0:q0 + n, MARGIN - 8:MARGIN - 8 + COMP, :] = r.reshape(n, COMP, 128) * hs[q0:q0 + n, MARGIN - 8:MARGIN - 8 + COMP, :]

    def n_chunk(s, q0, n, t, last):
        g0 = (q0 - first + k - 1 - s) // 2
        acc = conv_n(q0, n) + gate_n[s, g0:g0 + n // 2].reshape(n // 2 * COMP, 256)
        both = jnp.tanh(acc).reshape(n // 2, COMP, 256)
        cand = jnp.stack([both[:, :, :128], both[:, :, 128:]], axis=1).reshape(n, COMP, 128)
        h = hs[q0:q0 + n, MARGIN - 8:MARGIN - 8 + COMP, :]
        h_new = cand + zs[q0:q0 + n] * (h - cand)
        inner = h_new[:, 8:8 + width, :]
        for i in range(n):
            q = q0 + i - first
            keep = in_top if q < 0 else in_bottom if q >= n_pairs else None
            at = pl.ds(MARGIN, width)
            hs[q0 + i, at, :] = inner[i] if keep is None else jnp.where(keep, inner[i], 0.0)
            if not last:
                for lo, inside in ((0, in_left), (8 + width, in_right)):
                    inside = inside if keep is None else jnp.logical_and(inside, keep)
                    hs[q0 + i, MARGIN - 8 + lo:MARGIN + lo, :] = jnp.where(inside, h_new[i, lo:lo + 8, :], 0.0)
            if 0 <= q < n_pairs:
                seq_ref[t, q] = inner[i].T.astype(jnp.bfloat16)

    def chunks(lo, hi, size):
        for q0 in range(lo, hi, size):
            yield q0, min(size, hi - q0)

    n_sub = x_ref.shape[1]
    edge = halo * 8
    lane2 = lax.broadcasted_iota(jnp.int32, (1, 128), 1)

    def wide(v):
        return jnp.concatenate([v, jnp.zeros((v.shape[0], 128 - v.shape[1]), v.dtype)], axis=1)

    x_moves = DIRS + DIRS[:2]

    def x_copy(d):
        di, dj = x_moves[d]
        if dj == 0:
            frames = pl.ds(0, k) if d < 2 else pl.ds(k, n_steps - k)
            src = x_ref.at[frames, pl.ds(0 if di < 0 else n_sub - edge, edge), :]
            dst = x_row_in.at[0 if di < 0 else 1, frames]
        else:
            rows = {-1: pl.ds(0, edge), 1: pl.ds(n_sub - edge, edge), 0: pl.ds(0, n_sub)}[di]
            there_rows = {-1: pl.ds(edge + n_sub, edge), 1: pl.ds(0, edge), 0: pl.ds(edge, n_sub)}[di]
            side = 0 if dj < 0 else 1
            src = x_pack.at[side, rows, :]
            dst = x_col_in.at[side, there_rows, :]
        return pltpu.make_async_remote_copy(
            src_ref=src, dst_ref=dst, send_sem=x_send_sem.at[d], recv_sem=x_recv_sem.at[d],
            device_id=device(di, dj), device_id_type=pl.DeviceIdType.LOGICAL)

    def pack_x():
        for side in range(2):
            packed = jnp.zeros((n_sub, 128), jnp.float32)
            for t in range(n_steps):
                x = wide(x_ref[t].astype(jnp.float32))
                here = jnp.logical_and(lane2 >= 8 * t, lane2 < 8 * t + 8)
                packed = jnp.where(here, pltpu.roll(x, (8 * t - side * (width - 8)) % 128, 1), packed)
            x_pack[side] = packed.astype(jnp.bfloat16)

    def build_x(t, s):
        lo = lane2 < 8
        hi = lane2 >= 8 + width
        for first_sub, n, own, col in ((8, edge, x_row_in[1, t], 0), (8 + edge, n_sub, x_ref[t], edge), (8 + edge + n_sub, edge, x_row_in[0, t], edge + n_sub)):
            v = pltpu.roll(wide(own.astype(jnp.float32)), 8, 1)
            from_left = pltpu.roll(x_col_in[1, col:col + n, :].astype(jnp.float32), lax.rem(128 - 8 * t, 128), 1)
            from_right = pltpu.roll(x_col_in[0, col:col + n, :].astype(jnp.float32), lax.rem(128 + 8 + width - 8 * t, 128), 1)
            v = jnp.where(lo, from_left, jnp.where(hi, from_right, v))
            xs[0, first_sub:first_sub + n, :] = pltpu.roll(v, 1, 1)
            xs[1, first_sub:first_sub + n, :] = v
            xs[2, first_sub:first_sub + n, :] = pltpu.roll(v, 127, 1)
        zero = jnp.zeros((32, 128), jnp.bfloat16)
        for i in range(n_pairs + 2 * k):
            both = jnp.concatenate([xs[c, 16 * i:16 * i + 32].astype(jnp.bfloat16) for c in range(3)] + [zero], axis=0)
            xl[i] = both.T[:COMP]
        ext = k - 1 - s
        bias_zr = jnp.concatenate([b_ref[0:1, :], b_ref[1:2, :]], axis=1)
        bias_n = jnp.concatenate([b_ref[2:3, :], b_ref[2:3, :]], axis=1)
        for i, n in chunks(k - ext - 1, k + n_pairs + ext + 1, 2):
            part = jnp.dot(xl[i:i + n].reshape(n * COMP, 128), wxzr_ref[...], preferred_element_type=jnp.float32)
            gate_zr[s, i:i + n] = (part + bias_zr).reshape(n, COMP, 256)
        for g0, n in chunks(0, n_pairs // 2 + ext, 2):
            i = k - ext + 2 * g0
            two = xl[i:i + 2 * n].reshape(n, 2, COMP, 128)
            lhs = jnp.concatenate([two[:, 0], two[:, 1]], axis=-1).reshape(n * COMP, 256)
            part = jnp.dot(lhs, wxn_ref[...], preferred_element_type=jnp.float32)
            gate_n[s, g0:g0 + n] = (part + bias_n).reshape(n, COMP, 256)

    def fold_weights():
        def pair(get, a0, a1, gate):
            lo_part = get(a0, gate, 0) if 0 <= a0 <= 2 else None
            hi_part = get(a1, gate, 1) if 0 <= a1 <= 2 else None
            zero = jnp.zeros_like(lo_part if hi_part is None else hi_part)
            return jnp.where(lane2 < 64, zero if lo_part is None else lo_part, zero if hi_part is None else hi_part)

        for c in range(3):
            def get_h(a, gate, high):
                if gate == 2:
                    v = wide(whn_raw[a, c].astype(jnp.float32))
                    return pltpu.roll(v, 64, 1) if high else v
                v = whzr_raw[a, c].astype(jnp.float32)
                return pltpu.roll(v, 64, 1) if high != gate else v

            def get_x(a, gate, high):
                v = wx_raw[a, c].astype(jnp.float32)
                v = wide(v[:, 128:]) if gate == 2 else v[:, :128]
                return pltpu.roll(v, 64, 1) if high != (gate % 2) else v

            for j, rho in enumerate((0, 1, 2, -1)):
                at = c * 256 + j * 64
                for gate in range(2):
                    wzr_ref[at:at + 64, gate * 128:gate * 128 + 128] = pair(get_h, rho + 1, rho, gate).astype(jnp.bfloat16)
            for j, rho in enumerate((0, 1, 2, 3, 4, -1)):
                at = c * 384 + j * 64
                for o in (0, 2):
                    block = pair(get_h, rho - o + 1, rho - o, 2) if -1 <= rho - o <= 2 else jnp.zeros((64, 128), jnp.float32)
                    wn_ref[at:at + 64, o * 64:o * 64 + 128] = block.astype(jnp.bfloat16)
            for j, rho in enumerate((-1, 0, 1, 2)):
                at = c * 32 + j * 8
                for gate in range(3):
                    wx_ref[at:at + 8, gate * 128:gate * 128 + 128] = pair(get_x, rho + 1, rho, gate)
        wx_ref[96:128, :] = jnp.zeros((32, 384), jnp.float32)
        wxzr_ref[...] = wx_ref[:, :256].astype(jnp.bfloat16)
        wxn_ref[...] = jnp.zeros_like(wxn_ref)
        wxn_ref[0:128, 0:128] = wx_ref[:, 256:].astype(jnp.bfloat16)
        wxn_ref[128:256, 128:256] = wx_ref[:, 256:].astype(jnp.bfloat16)
        zr = bias_raw[:, :128]
        turned = pltpu.roll(zr, 64, 1)
        cand = wide(bias_raw[:, 128:])
        b_ref[0:1, :] = jnp.where(lane2 < 64, zr, turned)
        b_ref[1:2, :] = jnp.where(lane2 < 64, turned, zr)
        b_ref[2:3, :] = jnp.where(lane2 < 64, cand, pltpu.roll(cand, 64, 1))

    loads[0].wait()
    pack_x()
    pl.semaphore_wait(barrier, n_peers)

    def x_send(which):
        for d in which:
            @pl.when(there(*x_moves[d]))
            def _():
                x_copy(d).start()

    def x_receive(which, when):
        for d in which:
            @pl.when(jnp.logical_and(when, there(-x_moves[d][0], -x_moves[d][1])))
            def _():
                x_copy(d).wait_recv()

    x_send((4, 5, 6, 7, 2, 3, 0, 1))
    loads[1].wait()
    for q in range(n_pairs):
        hs[first + q, MARGIN:MARGIN + width, :] = h_ref[q].T
    send(0)
    x_send((8, 9))
    for load in loads[2:]:
        load.wait()
    fold_weights()
    xs[...] = jnp.zeros_like(xs)
    x_receive(range(8), my_row >= 0)

    def zr(s, lo, hi):
        for q0, n in chunks(first + lo, first + hi, CHUNK):
            zr_chunk(s, q0, n)

    def cand(t, s, lo, hi):
        for q0, n in chunks(first + lo, first + hi, N_CHUNK):
            n_chunk(s, q0, n, t, s == k - 1)

    n_periods = n_steps // k

    def period(p, carry):
        par = lax.rem(p, 2)
        for s in range(k):
            build_x(p * k + s, s)
        for s in range(k):
            ext = k - 1 - s
            t = p * k + s
            if s == 0:
                receive(par)
                x_receive((8, 9), p == 0)
                for m, (di, dj) in enumerate(moves):
                    @pl.when(there(di, dj))
                    def _():
                        move(m, par).wait_send()
                zr(s, -ext - 1, n_pairs + ext + 1)
            if s < k - 1:
                if s > 0:
                    zr(s, -ext - 1, n_pairs + ext + 1)
                cand(t, s, -ext, n_pairs + ext)
            else:
                more = p + 1 < n_periods

                if s > 0:
                    zr(s, -1, n_pairs + 1)
                cand(t, s, 0, n_pairs)

                @pl.when(more)
                def _():
                    send(1 - par)
        return carry

    lax.fori_loop(0, n_steps // k, period, 0)
    for q in range(n_pairs):
        last_ref[q] = hs[first + q, MARGIN:MARGIN + width, :].T
    for d, (di, dj) in enumerate(x_moves):
        @pl.when(there(di, dj))
        def _():
            x_copy(d).wait_send()


def solution(mesh):
    n_rows = mesh.shape['rows']
    n_cols = mesh.shape['cols']
    frame_spec = P(None, 'batch', 'rows', 'cols', None)
    state_spec = P('batch', 'rows', 'cols', None)

    def local_fn(frames, h_init, w_x, w_hzr, w_hn, gate_bias):
        n_steps, _, tile_h, width, c_in = frames.shape
        n_hidden = h_init.shape[-1]
        k = FUSE
        n_pairs = tile_h // 2
        x = frames[:, 0].transpose(0, 1, 3, 2).reshape(n_steps, tile_h * c_in, width)
        h0 = h_init[0].transpose(0, 2, 1).reshape(n_pairs, 2 * n_hidden, width)
        edge = 2 * k * c_in
        n_buf = n_pairs + 2 * k + 2
        vmem = pl.BlockSpec(memory_space=pltpu.VMEM)
        seq, last = pl.pallas_call(
            functools.partial(kernel, (n_steps, n_pairs, width, n_rows, n_cols)),
            out_shape=(pltpu.VMEM((n_steps, n_pairs, 128, width), jnp.bfloat16),
                       jax.ShapeDtypeStruct((n_pairs, 128, width), jnp.float32)),
            in_specs=[pl.BlockSpec(memory_space=pltpu.HBM)] * 6,
            out_specs=(vmem, vmem),
            scratch_shapes=[
                pltpu.VMEM(x.shape, x.dtype),
                pltpu.VMEM(h0.shape, h0.dtype),
                pltpu.VMEM(w_x.shape, w_x.dtype),
                pltpu.VMEM(w_hzr.shape, w_hzr.dtype),
                pltpu.VMEM(w_hn.shape, w_hn.dtype),
                pltpu.VMEM((1, gate_bias.shape[0]), gate_bias.dtype),
                pltpu.VMEM((n_buf, SUBLANES, 128), jnp.float32),
                pltpu.VMEM((n_buf, SUBLANES, 128), jnp.float32),
                pltpu.VMEM((n_buf, COMP, 128), jnp.float32),
                pltpu.VMEM((n_pairs + 2 * k, COMP, 128), jnp.bfloat16),
                pltpu.VMEM((k, n_pairs + 2 * k, COMP, 256), jnp.float32),
                pltpu.VMEM((k, n_pairs // 2 + k - 1, COMP, 256), jnp.float32),
                pltpu.VMEM((2, 2, k, width, 128), jnp.float32),
                pltpu.VMEM((2, 2, n_pairs, 2 * k, 128), jnp.float32),
                pltpu.VMEM((2, 4, k, 2 * k, 128), jnp.float32),
                pltpu.VMEM((768, 256), jnp.bfloat16),
                pltpu.VMEM((1152, 256), jnp.bfloat16),
                pltpu.VMEM((128, 384), jnp.float32),
                pltpu.VMEM((128, 256), jnp.bfloat16),
                pltpu.VMEM((256, 256), jnp.bfloat16),
                pltpu.VMEM((3, 128), jnp.float32),
                pltpu.VMEM((3, tile_h * c_in + 2 * edge + 16, 128), jnp.float32),
                pltpu.VMEM((2, tile_h * c_in, 128), jnp.bfloat16),
                pltpu.VMEM((2, n_steps, edge, width), jnp.bfloat16),
                pltpu.VMEM((2, tile_h * c_in + 2 * edge, 128), jnp.bfloat16),
                pltpu.SemaphoreType.DMA((8,)),
                pltpu.SemaphoreType.DMA((2, 8)),
                pltpu.SemaphoreType.DMA((10,)),
                pltpu.SemaphoreType.DMA((10,)),
                pltpu.SemaphoreType.DMA((6,)),
            ],
            compiler_params=pltpu.CompilerParams(collective_id=0, has_side_effects=True, vmem_limit_bytes=50 * 2**20),
        )(*[pltpu.with_memory_space_constraint(v, pltpu.HBM) for v in (x, h0, w_x, w_hzr, w_hn, gate_bias.reshape(1, -1))])
        seq = seq.reshape(n_steps, 1, tile_h, n_hidden, width).transpose(0, 1, 2, 4, 3)
        last = last.reshape(1, tile_h, n_hidden, width).transpose(0, 1, 3, 2)
        return seq, last

    return jax.shard_map(local_fn, mesh=mesh, in_specs=(frame_spec, state_spec, P(), P(), P(), P()), out_specs=(frame_spec, state_spec), check_vma=False)
```
